32 devices in a mesh: dp: 2 (over x), tp: 16 (over y, z, core).
Axes of the slice: x: 2, y: 2, z: 4, core: 2. Of those that a mesh axis runs over, the one named last changes fastest.
Arguments:
- x: bfloat16 [4096, 8192], P(('dp', 'tp')), parts along dimension 0
- dy: bfloat16 [4096, 8192], P(('dp', 'tp')), parts along dimension 0
- gain: bfloat16 [8192], replicated
- wq: bfloat16 [8192, 8192], P(None, 'tp')
- wk: bfloat16 [8192, 8192], P(None, 'tp')
- wv: bfloat16 [8192, 8192], P(None, 'tp')
- wo: bfloat16 [8192, 8192], P('tp')
Outputs:
- output 1: bfloat16 [4096, 8192], P(('dp', 'tp')), parts along dimension 0
- output 2: float32 [2, 8192], P('dp'), parts along dimension 0
- output 3: bfloat16 [16384, 8192], P('dp', 'tp'), parts along dimension 0
- output 4: bfloat16 [16384, 8192], P('dp', 'tp'), parts along dimension 0
- output 5: bfloat16 [16384, 8192], P('dp', 'tp'), parts along dimension 0
- output 6: bfloat16 [16384, 8192], P(('dp', 'tp')), parts along dimension 0
There are 2 independent parts. The reference program is written for one: setup_inputs(seed, part) draws one part's arguments, and reference() takes and returns one part's arrays. A program takes and returns all parts, laid end to end along the dimension named above; an argument that names none is the same for every part.
All inputs are finite; a program needn't handle non-finite values.
Results may differ from the reference program's by a relative error of at most 0.018.
Values are sent between devices in bfloat16 or wider.
A program may use at most 2 GiB of HBM per device.

```python
import jax
import jax.numpy as jnp
from jax import lax

ROWS = 2048
D = 8192
HEADS = 64
KV_HEADS = 64
HEAD = 128
THETA = 10000


def setup_inputs(seed: int = 0, part: int = 0) -> dict:
    kx, ky, kn, kq, kk, kv, ko = jax.random.split(jax.random.key(seed), 7)

    def weights(key, rows, columns):
        return jax.random.normal(key, (rows, columns), jnp.float32) * rows**-0.5

    drawn = {
        "x": jax.random.normal(jax.random.fold_in(kx, part), (ROWS, D), jnp.float32),
        "dy": jax.random.normal(jax.random.fold_in(ky, part), (ROWS, D), jnp.float32) * ROWS**-0.5,
        "gain": 1 + 0.1 * jax.random.normal(kn, (D,), jnp.float32),
        "wq": 2 * weights(kq, D, HEADS * HEAD),
        "wk": 2 * weights(kk, D, KV_HEADS * HEAD),
        "wv": 4 * weights(kv, D, KV_HEADS * HEAD),
        "wo": weights(ko, HEADS * HEAD, D),
    }
    return {k: v.astype(jnp.bfloat16) for k, v in drawn.items()}


def normed(x, gain):
    wide = x.astype(jnp.float32)
    scale = lax.rsqrt(jnp.mean(wide * wide, -1, keepdims=True) + 1e-6)
    return (wide * scale * gain.astype(jnp.float32)).astype(jnp.bfloat16)


def turned(t, place, theta):
    half = t.shape[-1] // 2
    angle = place.astype(jnp.float32)[:, None] * theta ** (-jnp.arange(half, dtype=jnp.float32) / half)
    cos, sin = jnp.cos(angle)[:, None], jnp.sin(angle)[:, None]
    a, b = t[..., :half].astype(jnp.float32), t[..., half:].astype(jnp.float32)
    return jnp.concatenate([a * cos - b * sin, b * cos + a * sin], -1).astype(jnp.bfloat16)


def matmul(a, w):
    return jnp.dot(a, w, preferred_element_type=jnp.float32).astype(jnp.bfloat16)


def einsum(form, a, b):
    return jnp.einsum(form, a.astype(jnp.float32), b.astype(jnp.float32))


def attention(q, k, v):
    scores = einsum("tgsd,ugd->gstu", q, k) * q.shape[-1] ** -0.5
    token = jnp.arange(q.shape[0])
    scores = jnp.where(token[:, None] >= token, scores, -jnp.inf)
    weights = jax.nn.softmax(scores, -1).astype(jnp.bfloat16)
    return einsum("gstu,ugd->tgsd", weights, v).astype(jnp.bfloat16)


def forward(x, gain, wq, wk, wv, wo):
    rows = x.shape[0]
    a, place = normed(x, gain), jnp.arange(rows)
    k = turned(matmul(a, wk).reshape(rows, -1, HEAD), place, THETA)
    q = turned(matmul(a, wq).reshape(rows, -1, HEAD), place, THETA).reshape(rows, k.shape[1], -1, HEAD)
    v = matmul(a, wv).reshape(rows, -1, HEAD)
    seen = attention(q, k, v).reshape(rows, -1)
    return (x.astype(jnp.float32) + jnp.dot(seen, wo, preferred_element_type=jnp.float32)).astype(jnp.bfloat16)


def reference(x, dy, gain, wq, wk, wv, wo):
    _, back = jax.vjp(forward, x, gain.astype(jnp.float32), wq, wk, wv, wo)
    by_x, by_gain, *by_weights = back(dy)
    return (by_x, by_gain[None], *by_weights)
```

```python
import jax
import jax.numpy as jnp
import numpy as np
from jax import lax
from jax.experimental import pallas as pl
from jax.experimental.pallas import tpu as pltpu
from jax.sharding import PartitionSpec as P

HEAD = 128
LOW = -1e30
HIDDEN = 2 * LOW
LOG2E = 1.4426950408889634
E2 = HEAD**-0.5 * LOG2E


def dot(a, b, ca, cb):
    return lax.dot_general(a, b, (((ca,), (cb,)), ((), ())), preferred_element_type=jnp.float32)


def head(h):
    return pl.ds(HEAD * h, HEAD)


def turn(t, cos, sin):
    half = HEAD // 2
    return t * cos + jnp.concatenate([t[:, half:], t[:, :half]], axis=1) * sin


def tables():
    rate = 10000.0 ** -(np.arange(HEAD) % (HEAD // 2) / (HEAD // 2))
    sign = np.where(np.arange(HEAD) < HEAD // 2, -1.0, 1.0)
    near, far = np.arange(128)[:, None] * rate, 128 * np.arange(16)[:, None] * rate
    return tuple(jnp.asarray(np.stack([np.cos(t), np.sin(t) * sign]), jnp.float32) for t in (near, far))


def angles(near_ref, far_ref, block):
    c, s = far_ref[0, pl.ds(block, 1), :], far_ref[1, pl.ds(block, 1), :]
    return near_ref[0] * c - near_ref[1] * s, near_ref[1] * c + near_ref[0] * s


def unit_angles(near_ref, far_ref, a, b):
    return tuple(jnp.concatenate(t, axis=0) for t in zip(angles(near_ref, far_ref, a), angles(near_ref, far_ref, b)))


MESH = pl.DeviceIdType.MESH
ANY = pl.BlockSpec(memory_space=pl.ANY)
VM = pl.BlockSpec(memory_space=pltpu.VMEM)
B16, F32 = jnp.bfloat16, jnp.float32
LIMIT = 67043328
GROUP = 16
BLOCK = 128


def dot(a, b, ca, cb):
    return lax.dot_general(a, b, (((ca,), (cb,)), ((), ())), preferred_element_type=jnp.float32)


def chip_at(r):
    far = r // 4
    return r * (1 - far) + (11 - r) * far


def part(i, size):
    return pl.ds(pl.multiple_of(i * size, size), size)


COLS = 2048
SLAB = 256
CHUNKS = 4
SENT = 7 * CHUNKS
ALL = 8 * CHUNKS


def copy_kernel(*refs):
    half = len(refs) // 2
    for a, b in zip(refs[:half], refs[half:]):
        b[...] = a[...]


UNIT = 2 * BLOCK
STEPS = 8
SPAN = 512


class Gather:
    def __init__(self, own_ref, out_ref, send_sem, recv_sem, sib_ssem, sib_rsem):
        self.own_ref, self.out_ref = own_ref, out_ref
        self.sems = send_sem, recv_sem, sib_ssem, sib_rsem
        group, me = lax.axis_index("dp"), lax.axis_index("tp")
        self.group, self.me = group, me
        self.core, self.r = lax.rem(me, 2), chip_at(me // 2)
        self.way = 1 - 2 * self.core
        self.sib = (group, me + self.way)
        self.succ, self.pred = ((group, chip_at(lax.rem(self.r + to + 8, 8)) * 2 + self.core) for to in (self.way, -self.way))

    def chip(self, far):
        return chip_at(lax.rem(self.r + far * self.way + 16, 8))

    def blocks(self, m):
        far, odd = (m + 1) // 2, lax.rem(m + 1, 2) * jnp.minimum(m, 1)
        return self.chip(-far) * 2 + self.core + odd * self.way, self.chip(far) * 2 + 1 - self.core - odd * self.way

    def ring(self, m, src=None):
        far, odd = (m - 1) // 2, lax.rem(m - 1, 2)
        there = part(self.chip(-far) * 2 + self.core + odd * self.way, BLOCK)
        return pltpu.make_async_remote_copy(src_ref=self.out_ref.at[there, :] if src is None else src, dst_ref=self.out_ref.at[there, :],
                                            send_sem=self.sems[0].at[m], recv_sem=self.sems[1].at[m], device_id=self.succ, device_id_type=MESH)

    def hand(self, m, src=None):
        there = part(self.blocks(m)[0], BLOCK)
        return pltpu.make_async_remote_copy(src_ref=self.out_ref.at[there, :] if src is None else src, dst_ref=self.out_ref.at[there, :],
                                            send_sem=self.sems[2].at[m], recv_sem=self.sems[3].at[m], device_id=self.sib, device_id_type=MESH)

    def start(self):
        self.ring(1, self.own_ref).start()
        self.hand(0, self.own_ref).start()

    def forward(self, m):
        self.ring(m).wait_recv()
        self.hand(m).start()

        @pl.when(m + 2 < STEPS)
        def _():
            self.ring(m + 2).start()

    def first(self):
        self.hand(0, self.own_ref).wait_recv()
        self.ring(2).start()

    def leave(self):
        self.ring(1, self.own_ref).wait_send()
        self.hand(0, self.own_ref).wait_send()

        @pl.loop(1, STEPS)
        def _(m):
            self.hand(m).wait_send()

            @pl.when(m >= 2)
            def _():
                self.ring(m).wait_send()


def project(gx, gy, x_ref, gain_s, ws, ax_ref, near_s, far_s, qkv_s, load_sem, w_sem, pair_sem, x_s, own_s, w_s, pair_s):
    wide, thin = ws[0].shape
    load = pltpu.make_async_copy(x_ref, x_s, load_sem.at[0])
    load.start()
    w_load = [pltpu.make_async_copy(w, w_s.at[n], w_sem.at[n, 0]) for n, w in enumerate(ws)]
    for c in w_load:
        c.start()
    load.wait()

    @pl.loop(0, BLOCK // 16)
    def _(i):
        x = x_s[part(i, 16), :].astype(F32)
        scale = lax.rsqrt(jnp.sum(x * x, -1, keepdims=True) * (1 / wide) + 1e-6)
        a = (x * scale * gain_s[...]).astype(B16)
        own_s[part(i, 16), :] = a
        pair_s[0, part(i, 16), :] = a

    pl.semaphore_wait(pltpu.get_barrier_semaphore(), GROUP - 1)
    gx.start()
    keep = pltpu.make_async_copy(own_s, ax_ref.at[part(gx.me, BLOCK), :], load_sem.at[0])
    keep.start()
    gx.first()

    @pl.loop(0, STEPS)
    def _(m):
        at = lax.rem(m, 2)
        a, b = gx.blocks(m)
        own, theirs = part(a, BLOCK), part(b, BLOCK)
        halves = [pltpu.make_async_copy(ax_ref.at[there, :], pair_s.at[at, pl.ds(n * BLOCK, BLOCK), :], pair_sem.at[n])
                  for n, there in enumerate((own, theirs))]

        @pl.when(m >= 1)
        def _():
            gx.forward(m)
            halves[0].start()

        @pl.when(m == STEPS - 3)
        def _():
            gy.start()

        @pl.when(m == STEPS - 2)
        def _():
            gy.first()

        @pl.when(m >= 1)
        def _():
            gx.hand(m).wait_recv()

        halves[1].start()

        @pl.when(m == 0)
        def _():
            for c in w_load:
                c.wait()

        @pl.when(m >= 1)
        def _():
            halves[0].wait()

        halves[1].wait()
        cos, sin = unit_angles(near_s, far_s, a, b)
        for n in range(3):
            t = dot(pair_s[at], w_s[n], 1, 0).astype(B16)
            if n < 2:
                t = jnp.concatenate([turn(t[:, c : c + HEAD].astype(F32), cos, sin).astype(B16) for c in range(0, thin, HEAD)], axis=1)
            qkv_s[own, pl.ds(thin * n, thin)] = t[:BLOCK]
            qkv_s[theirs, pl.ds(thin * n, thin)] = t[BLOCK:]

    keep.wait()
    gx.leave()


def attention(gy, dy_ref, wo_ref, ady_ref, dwo_ref, near_s, far_s, qkv_s, load_sem, pair_sem, out_sem,
              wo_s, seen_s, do_s, lse_s, top_s, mix_s, pair_s, seent_s, dwo_s, out_s, dq_s, dk_s, dv_s):
    load = pltpu.make_async_copy(wo_ref, wo_s, load_sem.at[0])
    load.start()
    rows, wide = qkv_s.shape[0], wo_s.shape[1]
    heads = wo_s.shape[0] // HEAD
    scale = HEAD**-0.5
    bq = SPAN
    ones = jnp.ones((8, bq), B16)

    @pl.loop(0, rows // bq)
    def _(iq):
        mine = part(iq, bq)
        top_s[...] = jnp.full_like(top_s, LOW)
        mix_s[...] = jnp.zeros_like(mix_s)

        def block(j, masked):
            here = part(j, bq)
            scores = [dot(qkv_s[here, head(heads + h)], qkv_s[mine, head(h)], 1, 1) for h in range(heads)]
            if masked:
                seen = lax.broadcasted_iota(jnp.int32, (bq, bq), 1) >= lax.broadcasted_iota(jnp.int32, (bq, bq), 0)
                scores = [jnp.where(seen, s, HIDDEN) for s in scores]
            weights, keeps = [], []
            for h, s in enumerate(scores):
                old = top_s[h : h + 1, :]
                top = jnp.maximum(old, s.max(axis=0, keepdims=True))
                top_s[h : h + 1, :] = top
                weights.append(jnp.exp2((s - top) * E2).astype(B16))
                keeps.append(jnp.exp2((old - top) * E2))
            for h, (p, keep) in enumerate(zip(weights, keeps)):
                values = jnp.concatenate([qkv_s[here, head(2 * heads + h)].T, ones], axis=0)
                mix_s[h] = mix_s[h] * keep + dot(values, p, 1, 0)

        lax.fori_loop(0, iq, lambda j, _: block(j, False), None)
        block(iq, True)
        for h in range(heads):
            total = mix_s[h, HEAD : HEAD + 1, :]
            seen_s[mine, head(h)] = (mix_s[h, :HEAD, :] * (1 / total)).T.astype(B16)
            lse_s[h : h + 1, mine] = top_s[h : h + 1, :] * E2 + jnp.log(total) * LOG2E

    gy.forward(1)
    dwo_s[...] = jnp.zeros_like(dwo_s)
    dk_s[...] = jnp.zeros_like(dk_s)
    dv_s[...] = jnp.zeros_like(dv_s)
    load.wait()

    def back(chip):
        mine = part(chip, UNIT)
        dq_s[...] = jnp.zeros_like(dq_s)
        deltas = [(do_s[mine, head(h)].astype(F32) * seen_s[mine, head(h)].astype(F32)).T.sum(axis=0, keepdims=True) for h in range(heads)]

        def block(j, masked):
            here = part(j, UNIT)
            scores = [dot(qkv_s[here, head(heads + h)], qkv_s[mine, head(h)], 1, 1) for h in range(heads)]
            dps = [dot(qkv_s[here, head(2 * heads + h)], do_s[mine, head(h)], 1, 1) for h in range(heads)]
            for h in range(heads):
                p = jnp.exp2(scores[h] * E2 - lse_s[h : h + 1, mine])
                if masked:
                    seen = lax.broadcasted_iota(jnp.int32, (UNIT, UNIT), 1) >= lax.broadcasted_iota(jnp.int32, (UNIT, UNIT), 0)
                    p = jnp.where(seen, p, 0.0)
                ds = (p * (dps[h] - deltas[h])).astype(B16)
                dv_s[here, head(h)] += dot(p.astype(B16), do_s[mine, head(h)], 1, 0)
                dk_s[here, head(h)] += dot(ds, qkv_s[mine, head(h)], 1, 0)
                dq_s[h] += dot(qkv_s[here, head(heads + h)].T, ds, 1, 0)

        lax.fori_loop(0, chip, lambda j, _: block(j, False), None)
        block(chip, True)
        cos, sin = unit_angles(near_s, far_s, 2 * chip, 2 * chip + 1)
        for h in range(heads):
            dq = (dq_s[h] * scale).T.astype(B16).astype(F32)
            qkv_s[mine, head(h)] = turn(dq, cos, -sin).astype(B16)

    def dwo_out(c):
        return pltpu.make_async_copy(out_s.at[lax.rem(c, 2)], dwo_ref.at[:, part(c, SPAN)], out_sem.at[lax.rem(c, 2)])

    @pl.loop(0, STEPS)
    def _(m):
        a, b = gy.blocks(m)
        own, theirs = part(a, BLOCK), part(b, BLOCK)
        halves = [pltpu.make_async_copy(from_ref, pair_s.at[pl.ds(n * BLOCK, BLOCK), :], pair_sem.at[n])
                  for n, from_ref in ((0, dy_ref), (0, ady_ref.at[own, :]), (1, ady_ref.at[theirs, :]))]

        @pl.when(m == 0)
        def _():
            halves[0].start()

        @pl.when(m >= 1)
        def _():
            halves[1].start()
            gy.hand(m).wait_recv()

        halves[2].start()
        seent_s[...] = jnp.concatenate([seen_s[own, :], seen_s[theirs, :]], axis=0).T
        halves[0].wait()
        halves[2].wait()
        t = dot(pair_s[...], wo_s[...], 1, 1).astype(B16)
        do_s[own, :] = t[:BLOCK]
        do_s[theirs, :] = t[BLOCK:]

        far = (m + 1) // 2

        @pl.loop(0, (1 - lax.rem(m, 2)) * (1 + jnp.minimum(m, 1)) + m // (STEPS - 1))
        def _(side):
            back(gy.chip(far * (2 * side - 1)))

        @pl.when(m < STEPS - 1)
        def _():
            @pl.loop(0, wide // SPAN)
            def _(c):
                dwo_s[:, part(c, SPAN)] += dot(seent_s[...], pair_s[:, part(c, SPAN)], 1, 0)

            @pl.when(m >= 1)
            def _():
                gy.forward(m + 1)

        @pl.when(m == STEPS - 1)
        def _():
            @pl.loop(0, wide // SPAN)
            def _(c):
                @pl.when(c >= 2)
                def _():
                    dwo_out(c - 2).wait()

                out_s[lax.rem(c, 2)] = (dwo_s[:, part(c, SPAN)] + dot(seent_s[...], pair_s[:, part(c, SPAN)], 1, 0)).astype(B16)
                dwo_out(c).start()

    @pl.loop(0, rows // UNIT)
    def _(i):
        here = part(i, UNIT)
        cos, sin = unit_angles(near_s, far_s, 2 * i, 2 * i + 1)
        for h in range(heads):
            dk = (dk_s[here, head(h)] * scale).astype(B16).astype(F32)
            qkv_s[here, head(heads + h)] = turn(dk, cos, -sin).astype(B16)
            qkv_s[here, head(2 * heads + h)] = dv_s[here, head(h)].astype(B16)

    for c in (wide // SPAN - 2, wide // SPAN - 1):
        dwo_out(c).wait()


def spread(gy, x_ref, dy_ref, gain_s, ws, ax_ref, bx_ref, bg_ref, dws, qkv_s, sib_in, run_in, gall_s,
           load_sem, w_sem, slab_sem, dw_sem, sib_ssem, sib_rsem, run_ssem, run_rsem, g_ssem, g_rsem, sib_free, run_free,
           w_s, slab_s, dw_s, own_s, sib_out, run_out, da_s, x_s, dy_s, gp_s, m_s, scale_s):
    group, me, core, r, way, sib, succ, pred = gy.group, gy.me, gy.core, gy.r, gy.way, gy.sib, gy.succ, gy.pred
    wide, thin = ws[0].shape
    piece = COLS // CHUNKS

    def w_load(n):
        return [pltpu.make_async_copy(w.at[part(n, piece), :], w_s.at[part(n, piece), pl.ds(thin * i, thin)], w_sem.at[i, n])
                for i, w in enumerate(ws)]

    def slab_load(k):
        return pltpu.make_async_copy(ax_ref.at[:, part(k, SLAB)], slab_s.at[lax.rem(k, 2)], slab_sem.at[lax.rem(k, 2)])

    @pl.loop(0, CHUNKS)
    def _(n):
        for c in w_load(n):
            c.start()

    slab_load(0).start()

    @pl.loop(CHUNKS, wide // piece)
    def _(n):
        for c in w_load(n):
            c.start()

    loads = [pltpu.make_async_copy(a, b, load_sem.at[i]) for i, (a, b) in enumerate(((x_ref, x_s), (dy_ref, dy_s)))]
    for c in loads:
        c.start()

    def sib_copy(k):
        at = lax.rem(k, 4)
        return pltpu.make_async_remote_copy(src_ref=sib_out.at[at], dst_ref=sib_in.at[at], send_sem=sib_ssem.at[at], recv_sem=sib_rsem.at[at],
                                            device_id=sib, device_id_type=MESH)

    def run_copy(k):
        a, b = lax.rem(k, 4), lax.rem(k, 8)
        return pltpu.make_async_remote_copy(src_ref=run_out.at[a], dst_ref=run_in.at[b], send_sem=run_ssem.at[a], recv_sem=run_rsem.at[b],
                                            device_id=succ, device_id_type=MESH)

    def gain_copy(j, n):
        return pltpu.make_async_remote_copy(src_ref=gall_s.at[j, me], dst_ref=gall_s.at[j, me], send_sem=g_ssem.at[j, n], recv_sem=g_rsem.at[j, n],
                                            device_id=(group, lax.rem(me + n, GROUP)), device_id_type=MESH)

    def term(k):
        s, j = k // CHUNKS, lax.rem(k, CHUNKS)
        mine = part(chip_at(lax.rem(r - way * (1 + s) + 16, 8)) * 2 + core, BLOCK)
        theirs = part(chip_at(lax.rem(r + way * (1 + s) + 16, 8)) * 2 + 1 - core, BLOCK)
        lhs = jnp.concatenate([qkv_s[mine, :], qkv_s[theirs, :]], axis=0)

        @pl.when(k >= 4)
        def _():
            sib_copy(k - 4).wait_send()
            pl.semaphore_wait(sib_free, 1)

        @pl.loop(0, CHUNKS)
        def _(n):
            @pl.when(k < CHUNKS)
            def _():
                for c in w_load(k * CHUNKS + n):
                    c.wait()

            t = dot(lhs, w_s[part(j * CHUNKS + n, piece), :], 1, 1)
            own_s[lax.rem(k, 2), :, part(n, piece)] = t[:BLOCK]
            sib_out[lax.rem(k, 4), :, part(n, piece)] = t[BLOCK:].astype(B16)

        sib_copy(k).start()

    def finish(k):
        sib_copy(k).wait_recv()

        def strips(write, with_run):
            @pl.loop(0, 8)
            def _(i):
                rows = part(i, 16)
                v = own_s[lax.rem(k, 2), rows, :] + sib_in[lax.rem(k, 4), rows, :].astype(F32)
                if with_run:
                    v += run_in[lax.rem(k + 4, 8), rows, :].astype(F32)
                write(rows, v)

        def to_run(rows, v):
            run_out[lax.rem(k, 4), rows, :] = v.astype(B16)

        here = part(lax.rem(k, CHUNKS), COLS)

        def to_da(rows, v):
            da_s[rows, here] = v
            t = v * (x_s[rows, here].astype(F32) * scale_s[rows, :1])
            gp_s[...] += t
            t = t * gain_s[:, here]
            m_s[rows, :] += sum(t[:, c : c + 128] for c in range(0, COLS, 128))

        @pl.when(k < 4)
        def _():
            strips(to_run, False)

        @pl.when(k >= 4)
        def _():
            run_copy(k - 4).wait_recv()

            @pl.when(k < SENT)
            def _():
                run_copy(k - 4).wait_send()
                strips(to_run, True)

            @pl.when(k >= SENT)
            def _():
                gp_s[...] = jnp.zeros_like(gp_s)
                strips(to_da, True)
                j = k - SENT
                share = COLS // 8
                for i in range(8):
                    gall_s[j, me, i : i + 1, :] = jnp.sum(gp_s[:, i * share : (i + 1) * share], axis=0, keepdims=True)
                for n in range(1, GROUP):
                    gain_copy(j, n).start()

            @pl.when(k < SENT - 4)
            def _():
                pl.semaphore_signal(run_free, inc=1, device_id=pred, device_id_type=MESH)

        @pl.when(k < ALL - 4)
        def _():
            pl.semaphore_signal(sib_free, inc=1, device_id=sib, device_id_type=MESH)

        @pl.when(k < SENT)
        def _():
            @pl.when(k >= 8)
            def _():
                pl.semaphore_wait(run_free, 1)

            run_copy(k).start()

    def dw_out(k, i):
        at = lax.rem(k, 2)
        return pltpu.make_async_copy(dw_s.at[at, i], dws[i].at[part(k, SLAB), :], dw_sem.at[at, i])

    def slab(k):
        at = lax.rem(k, 2)
        slab_load(k).wait()

        @pl.when(k + 1 < ALL)
        def _():
            slab_load(k + 1).start()

        @pl.when(k >= 2)
        def _():
            for i in range(3):
                dw_out(k - 2, i).wait()

        t = dot(slab_s[at], qkv_s[...], 0, 0)
        for i in range(3):
            dw_s[at, i] = t[:, thin * i : thin * (i + 1)].astype(B16)
            dw_out(k, i).start()

    term(0)

    @pl.loop(0, ALL)
    def _(k):
        @pl.when(k + 1 < ALL)
        def _():
            term(k + 1)

        @pl.loop(k * (jnp.minimum(k, 2) // 2), (k + 1) * jnp.minimum(k, 1))
        def _(n):
            slab(n)

        @pl.when(k == 8)
        def _():
            for c in loads:
                c.wait()
            m_s[...] = jnp.zeros_like(m_s)

            @pl.loop(0, BLOCK // 16)
            def _(i):
                x = x_s[part(i, 16), :].astype(F32)
                scale = lax.rsqrt(jnp.sum(x * x, -1, keepdims=True) * (1 / wide) + 1e-6)
                scale_s[part(i, 16), :] = jnp.broadcast_to(scale, (16, 128))

        finish(k)

    @pl.loop(0, BLOCK // 16)
    def _(i):
        rows = part(i, 16)
        scale = scale_s[rows, :1]
        m = jnp.sum(m_s[rows, :], -1, keepdims=True) * (1 / wide)
        u = da_s[rows, :] * gain_s[...] - x_s[rows, :].astype(F32) * (scale * m)
        x_s[rows, :] = (dy_s[rows, :].astype(F32) + scale * u).astype(B16)

    result = pltpu.make_async_copy(x_s, bx_ref, load_sem.at[0])
    result.start()
    for k in (ALL - 2, ALL - 1):
        for i in range(3):
            dw_out(k, i).wait()
    for k in range(ALL - 4, ALL):
        sib_copy(k).wait_send()
    for k in range(SENT - 4, SENT):
        run_copy(k).wait_send()

    @pl.loop(0, CHUNKS)
    def _(j):
        for n in range(1, GROUP):
            gain_copy(j, n).wait()

    for j in range(CHUNKS):
        v = sum(gall_s[j, n] for n in range(GROUP))
        share = COLS // 8
        for i in range(8):
            bg_ref[:, j * COLS + i * share : j * COLS + (i + 1) * share] = v[i : i + 1, :]
    result.wait()


def whole_kernel(x_ref, dy_ref, gain_ref, wq_ref, wk_ref, wv_ref, wo_ref, near_ref, far_ref,
                 bx_ref, bg_ref, dwq_ref, dwk_ref, dwv_ref, dwo_ref, ax_ref, ady_ref,
                 gain_s, near_s, far_s, qkv_s, sib_in, run_in, gall_s, load_sem, w_sem, pair_sem, out_sem, *sems):
    gx_sems, gy_sems, ring_sems = sems[:4], sems[4:8], sems[8:]
    gy = Gather(dy_ref, ady_ref, *gy_sems)
    barrier = pltpu.get_barrier_semaphore()
    for n in range(1, GROUP):
        pl.semaphore_signal(barrier, inc=1, device_id=(gy.group, lax.rem(gy.me + n, GROUP)), device_id_type=MESH)
    loads = [pltpu.make_async_copy(a, b, load_sem.at[1 + i]) for i, (a, b) in enumerate(((gain_ref, gain_s), (near_ref, near_s), (far_ref, far_s)))]
    for c in loads:
        c.start()
    for c in loads:
        c.wait()
    V = pltpu.VMEM
    ws, dws = (wq_ref, wk_ref, wv_ref), (dwq_ref, dwk_ref, dwv_ref)
    wide, thin = wq_ref.shape
    rows = qkv_s.shape[0]
    heads = thin // HEAD
    mine = V((BLOCK, wide), B16)
    pair = V((2, UNIT, wide), B16)
    chunks = lambda n: V((n, BLOCK, COLS), B16)

    def one(x_s, own_s, w_s, pair_s):
        gx = Gather(own_s, ax_ref, *gx_sems)
        project(gx, gy, x_ref, gain_s, ws, ax_ref, near_s, far_s, qkv_s, load_sem, w_sem, pair_sem, x_s, own_s, w_s, pair_s)

    pl.run_scoped(one, mine, mine, V((3, wide, thin), B16), pair)

    def two(*refs):
        attention(gy, dy_ref, wo_ref, ady_ref, dwo_ref, near_s, far_s, qkv_s, load_sem, pair_sem, out_sem, *refs)

    pl.run_scoped(two, V((thin, wide), B16), V((rows, thin), B16), V((rows, thin), B16), V((heads, rows), F32), V((heads, SPAN), F32),
                  V((heads, HEAD + 8, SPAN), F32), V((UNIT, wide), B16), V((thin, UNIT), B16), V((thin, wide), F32), V((2, thin, SPAN), B16),
                  V((heads, HEAD, UNIT), F32), V((rows, thin), F32), V((rows, thin), F32))

    def three(*refs):
        spread(gy, x_ref, dy_ref, gain_s, ws, ax_ref, bx_ref, bg_ref, dws, qkv_s, sib_in, run_in, gall_s, load_sem, w_sem, *ring_sems, *refs)

    pl.run_scoped(three, V((wide, 3 * thin), B16), V((2, rows, SLAB), B16), V((2, 3, SLAB, thin), B16), V((2, BLOCK, COLS), F32), chunks(4), chunks(4),
                  V((BLOCK, wide), F32), mine, mine, V((16, COLS), F32), V((BLOCK, 128), F32), V((BLOCK, 128), F32))
    gy.leave()


def whole(x, dy, gain, wq, wk, wv, wo):
    block, wide = x.shape
    rows, thin = GROUP * block, wq.shape[1]
    V, D = pltpu.VMEM, lambda *shape: pltpu.SemaphoreType.DMA(shape)
    S = jax.ShapeDtypeStruct
    near, far = tables()
    sem = pltpu.SemaphoreType.REGULAR
    bx, bg, *dw, _, _ = pl.pallas_call(
        whole_kernel,
        out_shape=[S(x.shape, B16), S((1, wide), F32)] + [S(wq.shape, B16)] * 3 + [S(wo.shape, B16)] + [S((rows, wide), B16)] * 2,
        in_specs=[ANY] * 9,
        out_specs=[ANY, VM] + [ANY] * 6,
        scratch_shapes=[V((1, wide), F32), V(near.shape, F32), V(far.shape, F32), V((rows, 3 * thin), B16), V((4, block, COLS), B16),
                        V((8, block, COLS), B16), V((CHUNKS, GROUP, 8, COLS // 8), F32), D(4), D(3, 16), D(2), D(2)]
                       + [D(STEPS)] * 8
                       + [D(2), D(2, 3), D(4), D(4), D(4), D(8), D(CHUNKS, GROUP), D(CHUNKS, GROUP), sem, sem],
        compiler_params=pltpu.CompilerParams(collective_id=0, has_side_effects=True, vmem_limit_bytes=LIMIT),
        cost_estimate=pl.CostEstimate(flops=22 * rows * thin * wide, bytes_accessed=8 * rows * wide, transcendentals=0),
        name="whole",
    )(x, dy, gain, wq, wk, wv, wo, near, far)
    steps = 8
    given = [bx, *dw]
    specs = [pl.BlockSpec((g.shape[0] // steps, g.shape[1]), lambda i: (i, 0)) for g in given] + [pl.BlockSpec(bg.shape, lambda i: (0, 0))]
    bx, *dw, bg = pl.pallas_call(copy_kernel, grid=(steps,), in_specs=specs, out_specs=specs, out_shape=[S(g.shape, g.dtype) for g in (*given, bg)],
                                 compiler_params=pltpu.CompilerParams(vmem_limit_bytes=LIMIT), name="results")(*given, bg)
    return bx, bg, *dw


def solution(mesh):
    def step(x, dy, gain, wq, wk, wv, wo):
        gain = gain.astype(F32)[None]
        return whole(x, dy, gain, wq, wk, wv, wo)

    tokens, columns = P(("dp", "tp"), None), P(None, "tp")
    return jax.shard_map(
        step,
        mesh=mesh,
        in_specs=(tokens, tokens, P(None), columns, columns, columns, P("tp", None)),
        out_specs=(tokens, P("dp", None), P("dp", "tp"), P("dp", "tp"), P("dp", "tp"), P(("dp", "tp"), None)),
        check_vma=False,
    )
```

```python
import jax
import jax.numpy as jnp
import numpy as np
from jax import lax
from jax.experimental import pallas as pl
from jax.experimental.pallas import tpu as pltpu
from jax.sharding import PartitionSpec as P

HEAD = 128
LOW = -1e30
HIDDEN = 2 * LOW
LOG2E = 1.4426950408889634
E2 = HEAD**-0.5 * LOG2E


def dot(a, b, ca, cb):
    return lax.dot_general(a, b, (((ca,), (cb,)), ((), ())), preferred_element_type=jnp.float32)


def head(h):
    return pl.ds(HEAD * h, HEAD)


def turn(t, cos, sin):
    half = HEAD // 2
    return t * cos + jnp.concatenate([t[:, half:], t[:, :half]], axis=1) * sin


def tables():
    rate = 10000.0 ** -(np.arange(HEAD) % (HEAD // 2) / (HEAD // 2))
    sign = np.where(np.arange(HEAD) < HEAD // 2, -1.0, 1.0)
    near, far = np.arange(128)[:, None] * rate, 128 * np.arange(16)[:, None] * rate
    return tuple(jnp.asarray(np.stack([np.cos(t), np.sin(t) * sign]), jnp.float32) for t in (near, far))


def angles(near_ref, far_ref, block):
    c, s = far_ref[0, pl.ds(block, 1), :], far_ref[1, pl.ds(block, 1), :]
    return near_ref[0] * c - near_ref[1] * s, near_ref[1] * c + near_ref[0] * s


def unit_angles(near_ref, far_ref, a, b):
    return tuple(jnp.concatenate(t, axis=0) for t in zip(angles(near_ref, far_ref, a), angles(near_ref, far_ref, b)))


MESH = pl.DeviceIdType.MESH
ANY = pl.BlockSpec(memory_space=pl.ANY)
VM = pl.BlockSpec(memory_space=pltpu.VMEM)
B16, F32 = jnp.bfloat16, jnp.float32
LIMIT = 67043328
GROUP = 16
BLOCK = 128


def dot(a, b, ca, cb):
    return lax.dot_general(a, b, (((ca,), (cb,)), ((), ())), preferred_element_type=jnp.float32)


def chip_at(r):
    far = r // 4
    return r * (1 - far) + (11 - r) * far


def part(i, size):
    return pl.ds(pl.multiple_of(i * size, size), size)


COLS = 2048
SLAB = 256
CHUNKS = 4
SENT = 7 * CHUNKS
ALL = 8 * CHUNKS


def copy_kernel(*refs):
    half = len(refs) // 2
    for a, b in zip(refs[:half], refs[half:]):
        b[...] = a[...]


UNIT = 2 * BLOCK
STEPS = 8
PIECES = 4
SPAN = 512


class Gather:
    def __init__(self, own_ref, out_ref, send_sem, recv_sem, sib_ssem, sib_rsem):
        self.own_ref, self.out_ref = own_ref, out_ref
        self.sems = send_sem, recv_sem, sib_ssem, sib_rsem
        group, me = lax.axis_index("dp"), lax.axis_index("tp")
        self.group, self.me = group, me
        self.core, self.r = lax.rem(me, 2), chip_at(me // 2)
        self.way = 1 - 2 * self.core
        self.sib = (group, me + self.way)
        self.succ, self.pred = ((group, chip_at(lax.rem(self.r + to + 8, 8)) * 2 + self.core) for to in (self.way, -self.way))

    def chip(self, far):
        return chip_at(lax.rem(self.r + far * self.way + 16, 8))

    def blocks(self, m):
        far, odd = (m + 1) // 2, lax.rem(m + 1, 2) * jnp.minimum(m, 1)
        return self.chip(-far) * 2 + self.core + odd * self.way, self.chip(far) * 2 + 1 - self.core - odd * self.way

    def copy(self, place, p, own, sems, m, to):
        there = self.out_ref.at[part(place * PIECES + p, BLOCK // PIECES), :]
        src = self.own_ref.at[part(p, BLOCK // PIECES), :] if own else there
        return pltpu.make_async_remote_copy(src_ref=src, dst_ref=there, send_sem=self.sems[sems].at[m, p], recv_sem=self.sems[sems + 1].at[m, p],
                                            device_id=to, device_id_type=MESH)

    def ring(self, m, p, own=False):
        far, odd = (m - 1) // 2, lax.rem(m - 1, 2)
        return self.copy(self.chip(-far) * 2 + self.core + odd * self.way, p, own, 0, m, self.succ)

    def hand(self, m, p, own=False):
        return self.copy(self.blocks(m)[0], p, own, 2, m, self.sib)

    def start(self, p):
        self.ring(1, p, True).start()
        self.hand(0, p, True).start()

    def forward(self, m):
        @pl.loop(0, PIECES)
        def _(p):
            self.ring(m, p).wait_recv()
            self.hand(m, p).start()

            @pl.when(m + 2 < STEPS)
            def _():
                self.ring(m + 2, p).start()

    def first(self):
        @pl.loop(0, PIECES)
        def _(p):
            self.hand(0, p, True).wait_recv()
            self.ring(2, p).start()

    def handed(self, m):
        @pl.loop(0, PIECES)
        def _(p):
            self.hand(m, p).wait_recv()

    def leave(self):
        @pl.loop(0, PIECES)
        def _(p):
            self.ring(1, p, True).wait_send()
            self.hand(0, p, True).wait_send()

            @pl.loop(1, STEPS)
            def _(m):
                self.hand(m, p).wait_send()

                @pl.when(m >= 2)
                def _():
                    self.ring(m, p).wait_send()


def project(gx, gy, small, x_ref, gain_raw, gain_s, ws, ax_ref, near_s, far_s, qkv_s, load_sem, w_sem, pair_sem, x_s, own_s, w_s, pair_s):
    wide, thin = ws[0].shape
    rows = BLOCK // PIECES
    load = [pltpu.make_async_copy(x_ref.at[part(p, rows), :], x_s.at[part(p, rows), :], load_sem.at[p]) for p in range(PIECES)]
    for c in load:
        c.start()
    for c in small:
        c.start()
    w_load = [pltpu.make_async_copy(w, w_s.at[n], w_sem.at[n, 0]) for n, w in enumerate(ws)]
    for c in w_load:
        c.start()
    for c in small:
        c.wait()
    gain = gain_raw[...].astype(F32)
    for n in range(wide // HEAD):
        gain_s[:, HEAD * n : HEAD * (n + 1)] = gain[n : n + 1, :]
    for p in range(PIECES):
        load[p].wait()

        @pl.loop(p * rows // 16, (p + 1) * rows // 16)
        def _(i):
            x = x_s[part(i, 16), :].astype(F32)
            scale = lax.rsqrt(jnp.sum(x * x, -1, keepdims=True) * (1 / wide) + 1e-6)
            a = (x * scale * gain_s[...]).astype(B16)
            own_s[part(i, 16), :] = a
            pair_s[0, part(i, 16), :] = a

        if p == 0:
            pl.semaphore_wait(pltpu.get_barrier_semaphore(), GROUP - 1)
        gx.start(p)
    keep = pltpu.make_async_copy(own_s, ax_ref.at[part(gx.me, BLOCK), :], load_sem.at[0])
    keep.start()
    gx.first()

    @pl.loop(0, STEPS)
    def _(m):
        at = lax.rem(m, 2)
        a, b = gx.blocks(m)
        own, theirs = part(a, BLOCK), part(b, BLOCK)
        halves = [pltpu.make_async_copy(ax_ref.at[there, :], pair_s.at[at, pl.ds(n * BLOCK, BLOCK), :], pair_sem.at[n])
                  for n, there in enumerate((own, theirs))]

        @pl.when(m >= 1)
        def _():
            gx.forward(m)
            halves[0].start()

        @pl.when(m == STEPS - 3)
        def _():
            for p in range(PIECES):
                gy.start(p)

        @pl.when(m == STEPS - 2)
        def _():
            gy.first()

        @pl.when(m >= 1)
        def _():
            gx.handed(m)

        halves[1].start()

        @pl.when(m == 0)
        def _():
            for c in w_load:
                c.wait()

        @pl.when(m >= 1)
        def _():
            halves[0].wait()

        halves[1].wait()
        cos, sin = unit_angles(near_s, far_s, a, b)
        for n in range(3):
            t = dot(pair_s[at], w_s[n], 1, 0).astype(B16)
            if n < 2:
                t = jnp.concatenate([turn(t[:, c : c + HEAD].astype(F32), cos, sin).astype(B16) for c in range(0, thin, HEAD)], axis=1)
            qkv_s[own, pl.ds(thin * n, thin)] = t[:BLOCK]
            qkv_s[theirs, pl.ds(thin * n, thin)] = t[BLOCK:]

    keep.wait()
    gx.leave()


def attention(gy, dy_ref, wo_ref, ady_ref, dwo_ref, near_s, far_s, qkv_s, load_sem, pair_sem, out_sem,
              wo_s, seen_s, do_s, lse_s, top_s, mix_s, pair_s, seent_s, dwo_s, out_s, dq_s, dk_s, dv_s):
    load = pltpu.make_async_copy(wo_ref, wo_s, load_sem.at[0])
    load.start()
    rows, wide = qkv_s.shape[0], wo_s.shape[1]
    heads = wo_s.shape[0] // HEAD
    scale = HEAD**-0.5
    bq = SPAN
    ones = jnp.ones((8, bq), B16)

    @pl.loop(0, rows // bq)
    def _(iq):
        mine = part(iq, bq)
        top_s[...] = jnp.full_like(top_s, LOW)
        mix_s[...] = jnp.zeros_like(mix_s)

        def block(j, masked):
            here = part(j, bq)
            scores = [dot(qkv_s[here, head(heads + h)], qkv_s[mine, head(h)], 1, 1) for h in range(heads)]
            if masked:
                seen = lax.broadcasted_iota(jnp.int32, (bq, bq), 1) >= lax.broadcasted_iota(jnp.int32, (bq, bq), 0)
                scores = [jnp.where(seen, s, HIDDEN) for s in scores]
            weights, keeps = [], []
            for h, s in enumerate(scores):
                old = top_s[h : h + 1, :]
                top = jnp.maximum(old, s.max(axis=0, keepdims=True))
                top_s[h : h + 1, :] = top
                weights.append(jnp.exp2((s - top) * E2).astype(B16))
                keeps.append(jnp.exp2((old - top) * E2))
            for h, (p, keep) in enumerate(zip(weights, keeps)):
                values = jnp.concatenate([qkv_s[here, head(2 * heads + h)].T, ones], axis=0)
                mix_s[h] = mix_s[h] * keep + dot(values, p, 1, 0)

        lax.fori_loop(0, iq, lambda j, _: block(j, False), None)
        block(iq, True)
        for h in range(heads):
            total = mix_s[h, HEAD : HEAD + 1, :]
            seen_s[mine, head(h)] = (mix_s[h, :HEAD, :] * (1 / total)).T.astype(B16)
            lse_s[h : h + 1, mine] = top_s[h : h + 1, :] * E2 + jnp.log(total) * LOG2E

    gy.forward(1)
    dwo_s[...] = jnp.zeros_like(dwo_s)
    dk_s[...] = jnp.zeros_like(dk_s)
    dv_s[...] = jnp.zeros_like(dv_s)
    load.wait()

    def back(chip):
        mine = part(chip, UNIT)
        dq_s[...] = jnp.zeros_like(dq_s)
        deltas = [(do_s[mine, head(h)].astype(F32) * seen_s[mine, head(h)].astype(F32)).T.sum(axis=0, keepdims=True) for h in range(heads)]

        def block(j, masked):
            here = part(j, UNIT)
            scores = [dot(qkv_s[here, head(heads + h)], qkv_s[mine, head(h)], 1, 1) for h in range(heads)]
            dps = [dot(qkv_s[here, head(2 * heads + h)], do_s[mine, head(h)], 1, 1) for h in range(heads)]
            for h in range(heads):
                p = jnp.exp2(scores[h] * E2 - lse_s[h : h + 1, mine])
                if masked:
                    seen = lax.broadcasted_iota(jnp.int32, (UNIT, UNIT), 1) >= lax.broadcasted_iota(jnp.int32, (UNIT, UNIT), 0)
                    p = jnp.where(seen, p, 0.0)
                ds = (p * (dps[h] - deltas[h])).astype(B16)
                dv_s[here, head(h)] += dot(p.astype(B16), do_s[mine, head(h)], 1, 0)
                dk_s[here, head(h)] += dot(ds, qkv_s[mine, head(h)], 1, 0)
                dq_s[h] += dot(qkv_s[here, head(heads + h)].T, ds, 1, 0)

        lax.fori_loop(0, chip, lambda j, _: block(j, False), None)
        block(chip, True)
        cos, sin = unit_angles(near_s, far_s, 2 * chip, 2 * chip + 1)
        for h in range(heads):
            dq = (dq_s[h] * scale).T.astype(B16).astype(F32)
            qkv_s[mine, head(h)] = turn(dq, cos, -sin).astype(B16)

    def own_half(m):
        return pltpu.make_async_copy(ady_ref.at[part(gy.blocks(m)[0], BLOCK), :], pair_s.at[pl.ds(0, BLOCK), :], pair_sem.at[0])

    pltpu.make_async_copy(dy_ref, pair_s.at[pl.ds(0, BLOCK), :], pair_sem.at[0]).start()

    def dwo_out(c):
        return pltpu.make_async_copy(out_s.at[lax.rem(c, 2)], dwo_ref.at[:, part(c, SPAN)], out_sem.at[lax.rem(c, 2)])

    @pl.loop(0, STEPS)
    def _(m):
        a, b = gy.blocks(m)
        own, theirs = part(a, BLOCK), part(b, BLOCK)
        their_half = pltpu.make_async_copy(ady_ref.at[theirs, :], pair_s.at[pl.ds(BLOCK, BLOCK), :], pair_sem.at[1])

        @pl.when(m >= 1)
        def _():
            gy.handed(m)

        their_half.start()
        seent_s[...] = jnp.concatenate([seen_s[own, :], seen_s[theirs, :]], axis=0).T
        own_half(m).wait()
        their_half.wait()
        t = dot(pair_s[...], wo_s[...], 1, 1).astype(B16)
        do_s[own, :] = t[:BLOCK]
        do_s[theirs, :] = t[BLOCK:]

        far = (m + 1) // 2

        @pl.loop(0, (1 - lax.rem(m, 2)) * (1 + jnp.minimum(m, 1)) + m // (STEPS - 1))
        def _(side):
            back(gy.chip(far * (2 * side - 1)))

        @pl.when(m < STEPS - 1)
        def _():
            @pl.loop(0, wide // (4 * SPAN))
            def _(c):
                for n in range(4):
                    here = pl.ds(pl.multiple_of(c * 4 * SPAN, 4 * SPAN) + n * SPAN, SPAN)
                    dwo_s[:, here] += dot(seent_s[...], pair_s[:, here], 1, 0)

            @pl.when(m >= 1)
            def _():
                gy.forward(m + 1)

            own_half(m + 1).start()

        @pl.when(m == STEPS - 1)
        def _():
            @pl.loop(0, wide // SPAN)
            def _(c):
                @pl.when(c >= 2)
                def _():
                    dwo_out(c - 2).wait()

                out_s[lax.rem(c, 2)] = (dwo_s[:, part(c, SPAN)] + dot(seent_s[...], pair_s[:, part(c, SPAN)], 1, 0)).astype(B16)
                dwo_out(c).start()

    @pl.loop(0, rows // UNIT)
    def _(i):
        here = part(i, UNIT)
        cos, sin = unit_angles(near_s, far_s, 2 * i, 2 * i + 1)
        for h in range(heads):
            dk = (dk_s[here, head(h)] * scale).astype(B16).astype(F32)
            qkv_s[here, head(heads + h)] = turn(dk, cos, -sin).astype(B16)
            qkv_s[here, head(2 * heads + h)] = dv_s[here, head(h)].astype(B16)

    for c in (wide // SPAN - 2, wide // SPAN - 1):
        dwo_out(c).wait()


def spread(gy, x_ref, dy_ref, gain_s, ws, ax_ref, bx_ref, bg_ref, dws, qkv_s, sib_in, run_in, gall_s,
           load_sem, w_sem, slab_sem, dw_sem, sib_ssem, sib_rsem, run_ssem, run_rsem, g_ssem, g_rsem, sib_free, run_free,
           w_s, slab_s, dw_s, own_s, sib_out, run_out, da_s, x_s, dy_s, gp_s, m_s, scale_s):
    group, me, core, r, way, sib, succ, pred = gy.group, gy.me, gy.core, gy.r, gy.way, gy.sib, gy.succ, gy.pred
    wide, thin = ws[0].shape
    piece = COLS // CHUNKS

    def w_load(n):
        return [pltpu.make_async_copy(w.at[part(n, piece), :], w_s.at[part(n, piece), pl.ds(thin * i, thin)], w_sem.at[i, n])
                for i, w in enumerate(ws)]

    def slab_load(k):
        return pltpu.make_async_copy(ax_ref.at[:, part(k, SLAB)], slab_s.at[lax.rem(k, 2)], slab_sem.at[lax.rem(k, 2)])

    @pl.loop(0, CHUNKS)
    def _(n):
        for c in w_load(n):
            c.start()

    slab_load(0).start()

    @pl.loop(CHUNKS, wide // piece)
    def _(n):
        for c in w_load(n):
            c.start()

    loads = [pltpu.make_async_copy(a, b, load_sem.at[i]) for i, (a, b) in enumerate(((x_ref, x_s), (dy_ref, dy_s)))]
    for c in loads:
        c.start()

    def sib_copy(k):
        at = lax.rem(k, 4)
        return pltpu.make_async_remote_copy(src_ref=sib_out.at[at], dst_ref=sib_in.at[at], send_sem=sib_ssem.at[at], recv_sem=sib_rsem.at[at],
                                            device_id=sib, device_id_type=MESH)

    def run_copy(k):
        a, b = lax.rem(k, 4), lax.rem(k, 8)
        return pltpu.make_async_remote_copy(src_ref=run_out.at[a], dst_ref=run_in.at[b], send_sem=run_ssem.at[a], recv_sem=run_rsem.at[b],
                                            device_id=succ, device_id_type=MESH)

    def gain_copy(j, n):
        return pltpu.make_async_remote_copy(src_ref=gall_s.at[j, me], dst_ref=gall_s.at[j, me], send_sem=g_ssem.at[j, n], recv_sem=g_rsem.at[j, n],
                                            device_id=(group, lax.rem(me + n, GROUP)), device_id_type=MESH)

    def term(k):
        s, j = k // CHUNKS, lax.rem(k, CHUNKS)
        mine = part(chip_at(lax.rem(r - way * (1 + s) + 16, 8)) * 2 + core, BLOCK)
        theirs = part(chip_at(lax.rem(r + way * (1 + s) + 16, 8)) * 2 + 1 - core, BLOCK)
        lhs = jnp.concatenate([qkv_s[mine, :], qkv_s[theirs, :]], axis=0)

        @pl.when(k >= 4)
        def _():
            sib_copy(k - 4).wait_send()
            pl.semaphore_wait(sib_free, 1)

        @pl.loop(0, CHUNKS)
        def _(n):
            @pl.when(k < CHUNKS)
            def _():
                for c in w_load(k * CHUNKS + n):
                    c.wait()

            t = dot(lhs, w_s[part(j * CHUNKS + n, piece), :], 1, 1)
            own_s[lax.rem(k, 2), :, part(n, piece)] = t[:BLOCK]
            sib_out[lax.rem(k, 4), :, part(n, piece)] = t[BLOCK:].astype(B16)

        sib_copy(k).start()

    def finish(k):
        sib_copy(k).wait_recv()

        def strips(write, with_run):
            @pl.loop(0, 8)
            def _(i):
                rows = part(i, 16)
                v = own_s[lax.rem(k, 2), rows, :] + sib_in[lax.rem(k, 4), rows, :].astype(F32)
                if with_run:
                    v += run_in[lax.rem(k + 4, 8), rows, :].astype(F32)
                write(rows, v)

        def to_run(rows, v):
            run_out[lax.rem(k, 4), rows, :] = v.astype(B16)

        here = part(lax.rem(k, CHUNKS), COLS)

        def to_da(rows, v):
            da_s[rows, here] = v
            t = v * (x_s[rows, here].astype(F32) * scale_s[rows, :1])
            gp_s[...] += t
            t = t * gain_s[:, here]
            m_s[rows, :] += sum(t[:, c : c + 128] for c in range(0, COLS, 128))

        @pl.when(k < 4)
        def _():
            strips(to_run, False)

        @pl.when(k >= 4)
        def _():
            run_copy(k - 4).wait_recv()

            @pl.when(k < SENT)
            def _():
                run_copy(k - 4).wait_send()
                strips(to_run, True)

            @pl.when(k >= SENT)
            def _():
                gp_s[...] = jnp.zeros_like(gp_s)
                strips(to_da, True)
                j = k - SENT
                share = COLS // 8
                for i in range(8):
                    gall_s[j, me, i : i + 1, :] = jnp.sum(gp_s[:, i * share : (i + 1) * share], axis=0, keepdims=True)
                for n in range(1, GROUP):
                    gain_copy(j, n).start()

            @pl.when(k < SENT - 4)
            def _():
                pl.semaphore_signal(run_free, inc=1, device_id=pred, device_id_type=MESH)

        @pl.when(k < ALL - 4)
        def _():
            pl.semaphore_signal(sib_free, inc=1, device_id=sib, device_id_type=MESH)

        @pl.when(k < SENT)
        def _():
            @pl.when(k >= 8)
            def _():
                pl.semaphore_wait(run_free, 1)

            run_copy(k).start()

    def dw_out(k, i):
        at = lax.rem(k, 2)
        return pltpu.make_async_copy(dw_s.at[at, i], dws[i].at[part(k, SLAB), :], dw_sem.at[at, i])

    def slab(k):
        at = lax.rem(k, 2)
        slab_load(k).wait()

        @pl.when(k + 1 < ALL)
        def _():
            slab_load(k + 1).start()

        @pl.when(k >= 2)
        def _():
            for i in range(3):
                dw_out(k - 2, i).wait()

        t = dot(slab_s[at], qkv_s[...], 0, 0)
        for i in range(3):
            dw_s[at, i] = t[:, thin * i : thin * (i + 1)].astype(B16)
            dw_out(k, i).start()

    term(0)

    @pl.loop(0, ALL)
    def _(k):
        @pl.when(k + 1 < ALL)
        def _():
            term(k + 1)

        @pl.loop(k * (jnp.minimum(k, 2) // 2), (k + 1) * jnp.minimum(k, 1))
        def _(n):
            slab(n)

        @pl.when(k == 8)
        def _():
            for c in loads:
                c.wait()
            m_s[...] = jnp.zeros_like(m_s)

            @pl.loop(0, BLOCK // 16)
            def _(i):
                x = x_s[part(i, 16), :].astype(F32)
                scale = lax.rsqrt(jnp.sum(x * x, -1, keepdims=True) * (1 / wide) + 1e-6)
                scale_s[part(i, 16), :] = jnp.broadcast_to(scale, (16, 128))

        finish(k)

    @pl.loop(0, BLOCK // 16)
    def _(i):
        rows = part(i, 16)
        scale = scale_s[rows, :1]
        m = jnp.sum(m_s[rows, :], -1, keepdims=True) * (1 / wide)
        u = da_s[rows, :] * gain_s[...] - x_s[rows, :].astype(F32) * (scale * m)
        x_s[rows, :] = (dy_s[rows, :].astype(F32) + scale * u).astype(B16)
        pltpu.make_async_copy(x_s.at[rows, :], bx_ref.at[rows, :], load_sem.at[i]).start()

    for k in (ALL - 2, ALL - 1):
        for i in range(3):
            dw_out(k, i).wait()
    for k in range(ALL - 4, ALL):
        sib_copy(k).wait_send()
    for k in range(SENT - 4, SENT):
        run_copy(k).wait_send()

    @pl.loop(0, CHUNKS)
    def _(j):
        for n in range(1, GROUP):
            gain_copy(j, n).wait()

    for j in range(CHUNKS):
        v = sum(gall_s[j, n] for n in range(GROUP))
        share = COLS // 8
        for i in range(8):
            bg_ref[:, j * COLS + i * share : j * COLS + (i + 1) * share] = v[i : i + 1, :]
    @pl.loop(0, BLOCK // 16)
    def _(i):
        pltpu.make_async_copy(x_s.at[part(i, 16), :], bx_ref.at[part(i, 16), :], load_sem.at[i]).wait()


def whole_kernel(x_ref, dy_ref, gain_ref, wq_ref, wk_ref, wv_ref, wo_ref, near_ref, far_ref,
                 bx_ref, bg_ref, dwq_ref, dwk_ref, dwv_ref, dwo_ref, ax_ref, ady_ref,
                 gain_raw, gain_s, near_s, far_s, qkv_s, sib_in, run_in, gall_s, load_sem, w_sem, pair_sem, out_sem, *sems):
    gx_sems, gy_sems, ring_sems = sems[:4], sems[4:8], sems[8:]
    gy = Gather(dy_ref, ady_ref, *gy_sems)
    barrier = pltpu.get_barrier_semaphore()
    for n in range(1, GROUP):
        pl.semaphore_signal(barrier, inc=1, device_id=(gy.group, lax.rem(gy.me + n, GROUP)), device_id_type=MESH)
    small = [pltpu.make_async_copy(a, b, load_sem.at[PIECES + i]) for i, (a, b) in enumerate(((gain_ref, gain_raw), (near_ref, near_s), (far_ref, far_s)))]
    V = pltpu.VMEM
    ws, dws = (wq_ref, wk_ref, wv_ref), (dwq_ref, dwk_ref, dwv_ref)
    wide, thin = wq_ref.shape
    rows = qkv_s.shape[0]
    heads = thin // HEAD
    mine = V((BLOCK, wide), B16)
    pair = V((2, UNIT, wide), B16)
    chunks = lambda n: V((n, BLOCK, COLS), B16)

    def one(x_s, own_s, w_s, pair_s):
        gx = Gather(own_s, ax_ref, *gx_sems)
        project(gx, gy, small, x_ref, gain_raw, gain_s, ws, ax_ref, near_s, far_s, qkv_s, load_sem, w_sem, pair_sem, x_s, own_s, w_s, pair_s)

    pl.run_scoped(one, mine, mine, V((3, wide, thin), B16), pair)

    def two(*refs):
        attention(gy, dy_ref, wo_ref, ady_ref, dwo_ref, near_s, far_s, qkv_s, load_sem, pair_sem, out_sem, *refs)

    pl.run_scoped(two, V((thin, wide), B16), V((rows, thin), B16), V((rows, thin), B16), V((heads, rows), F32), V((heads, SPAN), F32),
                  V((heads, HEAD + 8, SPAN), F32), V((UNIT, wide), B16), V((thin, UNIT), B16), V((thin, wide), F32), V((2, thin, SPAN), B16),
                  V((heads, HEAD, UNIT), F32), V((rows, thin), F32), V((rows, thin), F32))

    def three(*refs):
        spread(gy, x_ref, dy_ref, gain_s, ws, ax_ref, bx_ref, bg_ref, dws, qkv_s, sib_in, run_in, gall_s, load_sem, w_sem, *ring_sems, *refs)

    pl.run_scoped(three, V((wide, 3 * thin), B16), V((2, rows, SLAB), B16), V((2, 3, SLAB, thin), B16), V((2, BLOCK, COLS), F32), chunks(4), chunks(4),
                  V((BLOCK, wide), F32), mine, mine, V((16, COLS), F32), V((BLOCK, 128), F32), V((BLOCK, 128), F32))
    gy.leave()


def whole(x, dy, gain, wq, wk, wv, wo):
    block, wide = x.shape
    rows, thin = GROUP * block, wq.shape[1]
    V, D = pltpu.VMEM, lambda *shape: pltpu.SemaphoreType.DMA(shape)
    S = jax.ShapeDtypeStruct
    near, far = tables()
    sem = pltpu.SemaphoreType.REGULAR
    bx, bg, *dw, _, _ = pl.pallas_call(
        whole_kernel,
        out_shape=[S(x.shape, B16), S((1, wide), F32)] + [S(wq.shape, B16)] * 3 + [S(wo.shape, B16)] + [S((rows, wide), B16)] * 2,
        in_specs=[ANY] * 9,
        out_specs=[ANY, VM] + [ANY] * 6,
        scratch_shapes=[V(gain.shape, B16), V((1, wide), F32), V(near.shape, F32), V(far.shape, F32), V((rows, 3 * thin), B16), V((4, block, COLS), B16),
                        V((8, block, COLS), B16), V((CHUNKS, GROUP, 8, COLS // 8), F32), D(8), D(3, 16), D(2), D(2)]
                       + [D(STEPS, PIECES)] * 8
                       + [D(2), D(2, 3), D(4), D(4), D(4), D(8), D(CHUNKS, GROUP), D(CHUNKS, GROUP), sem, sem],
        compiler_params=pltpu.CompilerParams(collective_id=0, has_side_effects=True, vmem_limit_bytes=LIMIT),
        cost_estimate=pl.CostEstimate(flops=22 * rows * thin * wide, bytes_accessed=8 * rows * wide, transcendentals=0),
        name="whole",
    )(x, dy, gain, wq, wk, wv, wo, near, far)
    steps = 8
    given = [bx, *dw]
    specs = [pl.BlockSpec((g.shape[0] // steps, g.shape[1]), lambda i: (i, 0)) for g in given] + [pl.BlockSpec(bg.shape, lambda i: (0, 0))]
    bx, *dw, bg = pl.pallas_call(copy_kernel, grid=(steps,), in_specs=specs, out_specs=specs, out_shape=[S(g.shape, g.dtype) for g in (*given, bg)],
                                 compiler_params=pltpu.CompilerParams(vmem_limit_bytes=LIMIT), name="results")(*given, bg)
    return bx, bg, *dw


def solution(mesh):
    def step(x, dy, gain, wq, wk, wv, wo):
        gain = gain.reshape(-1, HEAD)
        return whole(x, dy, gain, wq, wk, wv, wo)

    tokens, columns = P(("dp", "tp"), None), P(None, "tp")
    return jax.shard_map(
        step,
        mesh=mesh,
        in_specs=(tokens, tokens, P(None), columns, columns, columns, P("tp", None)),
        out_specs=(tokens, P("dp", None), P("dp", "tp"), P("dp", "tp"), P("dp", "tp"), P(("dp", "tp"), None)),
        check_vma=False,
    )
```

```python
import jax
import jax.numpy as jnp
import numpy as np
from jax import lax
from jax.experimental import pallas as pl
from jax.experimental.pallas import tpu as pltpu
from jax.sharding import PartitionSpec as P

HEAD = 128
LOW = -1e30
HIDDEN = 2 * LOW
LOG2E = 1.4426950408889634
E2 = HEAD**-0.5 * LOG2E


def dot(a, b, ca, cb):
    return lax.dot_general(a, b, (((ca,), (cb,)), ((), ())), preferred_element_type=jnp.float32)


def head(h):
    return pl.ds(HEAD * h, HEAD)


def turn(t, cos, sin):
    half = HEAD // 2
    return t * cos + jnp.concatenate([t[:, half:], t[:, :half]], axis=1) * sin


def tables():
    rate = 10000.0 ** -(np.arange(HEAD) % (HEAD // 2) / (HEAD // 2))
    sign = np.where(np.arange(HEAD) < HEAD // 2, -1.0, 1.0)
    near, far = np.arange(128)[:, None] * rate, 128 * np.arange(16)[:, None] * rate
    return tuple(jnp.asarray(np.stack([np.cos(t), np.sin(t) * sign]), jnp.float32) for t in (near, far))


def angles(near_ref, far_ref, block):
    c, s = far_ref[0, pl.ds(block, 1), :], far_ref[1, pl.ds(block, 1), :]
    return near_ref[0] * c - near_ref[1] * s, near_ref[1] * c + near_ref[0] * s


def unit_angles(near_ref, far_ref, a, b):
    return tuple(jnp.concatenate(t, axis=0) for t in zip(angles(near_ref, far_ref, a), angles(near_ref, far_ref, b)))


MESH = pl.DeviceIdType.MESH
ANY = pl.BlockSpec(memory_space=pl.ANY)
VM = pl.BlockSpec(memory_space=pltpu.VMEM)
B16, F32 = jnp.bfloat16, jnp.float32
LIMIT = 67043328
GROUP = 16
BLOCK = 128


def dot(a, b, ca, cb):
    return lax.dot_general(a, b, (((ca,), (cb,)), ((), ())), preferred_element_type=jnp.float32)


def chip_at(r):
    far = r // 4
    return r * (1 - far) + (11 - r) * far


def part(i, size):
    return pl.ds(pl.multiple_of(i * size, size), size)


COLS = 2048
SLAB = 256
CHUNKS = 4
SENT = 7 * CHUNKS
ALL = 8 * CHUNKS


def copy_kernel(*refs):
    half = len(refs) // 2
    for a, b in zip(refs[:half], refs[half:]):
        b[...] = a[...]


UNIT = 2 * BLOCK
STEPS = 8
PIECES = 4
SPAN = 512


class Gather:
    def __init__(self, own_ref, out_ref, send_sem, recv_sem, sib_ssem, sib_rsem):
        self.own_ref, self.out_ref = own_ref, out_ref
        self.sems = send_sem, recv_sem, sib_ssem, sib_rsem
        group, me = lax.axis_index("dp"), lax.axis_index("tp")
        self.group, self.me = group, me
        self.core, self.r = lax.rem(me, 2), chip_at(me // 2)
        self.way = 1 - 2 * self.core
        self.sib = (group, me + self.way)
        self.succ, self.pred = ((group, chip_at(lax.rem(self.r + to + 8, 8)) * 2 + self.core) for to in (self.way, -self.way))

    def chip(self, far):
        return chip_at(lax.rem(self.r + far * self.way + 16, 8))

    def blocks(self, m):
        far, odd = (m + 1) // 2, lax.rem(m + 1, 2) * jnp.minimum(m, 1)
        return self.chip(-far) * 2 + self.core + odd * self.way, self.chip(far) * 2 + 1 - self.core - odd * self.way

    def copy(self, place, p, own, sems, m, to):
        there = self.out_ref.at[part(place * PIECES + p, BLOCK // PIECES), :]
        src = self.own_ref.at[part(p, BLOCK // PIECES), :] if own else there
        return pltpu.make_async_remote_copy(src_ref=src, dst_ref=there, send_sem=self.sems[sems].at[m, p], recv_sem=self.sems[sems + 1].at[m, p],
                                            device_id=to, device_id_type=MESH)

    def ring(self, m, p, own=False):
        far, odd = (m - 1) // 2, lax.rem(m - 1, 2)
        return self.copy(self.chip(-far) * 2 + self.core + odd * self.way, p, own, 0, m, self.succ)

    def hand(self, m, p, own=False):
        return self.copy(self.blocks(m)[0], p, own, 2, m, self.sib)

    def start(self, p):
        self.ring(1, p, True).start()
        self.hand(0, p, True).start()

    def forward(self, m):
        @pl.loop(0, PIECES)
        def _(p):
            self.ring(m, p).wait_recv()
            self.hand(m, p).start()

            @pl.when(m + 2 < STEPS)
            def _():
                self.ring(m + 2, p).start()

    def first(self):
        @pl.loop(0, PIECES)
        def _(p):
            self.hand(0, p, True).wait_recv()
            self.ring(2, p).start()

    def handed(self, m):
        @pl.loop(0, PIECES)
        def _(p):
            self.hand(m, p).wait_recv()

    def leave(self):
        @pl.loop(0, PIECES)
        def _(p):
            self.ring(1, p, True).wait_send()
            self.hand(0, p, True).wait_send()

            @pl.loop(1, STEPS)
            def _(m):
                self.hand(m, p).wait_send()

                @pl.when(m >= 2)
                def _():
                    self.ring(m, p).wait_send()


def project(gx, gy, small, x_ref, gain_raw, gain_s, ws, ax_ref, near_s, far_s, qkv_s, load_sem, w_sem, pair_sem, x_s, own_s, w_s, pair_s):
    wide, thin = ws[0].shape
    rows = BLOCK // PIECES
    load = [pltpu.make_async_copy(x_ref.at[part(p, rows), :], x_s.at[part(p, rows), :], load_sem.at[p]) for p in range(PIECES)]
    for c in load:
        c.start()
    for c in small:
        c.start()
    w_load = [pltpu.make_async_copy(w, w_s.at[n], w_sem.at[n, 0]) for n, w in enumerate(ws)]
    for c in w_load:
        c.start()
    for c in small:
        c.wait()
    gain = gain_raw[...].astype(F32)
    for n in range(wide // HEAD):
        gain_s[:, HEAD * n : HEAD * (n + 1)] = gain[n : n + 1, :]
    for p in range(PIECES):
        load[p].wait()

        @pl.loop(p * rows // 16, (p + 1) * rows // 16)
        def _(i):
            x = x_s[part(i, 16), :].astype(F32)
            scale = lax.rsqrt(jnp.sum(x * x, -1, keepdims=True) * (1 / wide) + 1e-6)
            a = (x * scale * gain_s[...]).astype(B16)
            own_s[part(i, 16), :] = a
            pair_s[0, part(i, 16), :] = a

        if p == 0:
            pl.semaphore_wait(pltpu.get_barrier_semaphore(), GROUP - 1)
        gx.start(p)
    keep = pltpu.make_async_copy(own_s, ax_ref.at[part(gx.me, BLOCK), :], load_sem.at[0])
    keep.start()
    gx.first()

    @pl.loop(0, STEPS)
    def _(m):
        at = lax.rem(m, 2)
        a, b = gx.blocks(m)
        own, theirs = part(a, BLOCK), part(b, BLOCK)
        halves = [pltpu.make_async_copy(ax_ref.at[there, :], pair_s.at[at, pl.ds(n * BLOCK, BLOCK), :], pair_sem.at[n])
                  for n, there in enumerate((own, theirs))]

        @pl.when(m >= 1)
        def _():
            gx.forward(m)
            halves[0].start()

        @pl.when(m == STEPS - 3)
        def _():
            for p in range(PIECES):
                gy.start(p)

        @pl.when(m == STEPS - 2)
        def _():
            gy.first()

        @pl.when(m >= 1)
        def _():
            gx.handed(m)

        halves[1].start()

        @pl.when(m == 0)
        def _():
            for c in w_load:
                c.wait()

        @pl.when(m >= 1)
        def _():
            halves[0].wait()

        halves[1].wait()
        cos, sin = unit_angles(near_s, far_s, a, b)
        for n in range(3):
            t = dot(pair_s[at], w_s[n], 1, 0).astype(B16)
            if n < 2:
                t = jnp.concatenate([turn(t[:, c : c + HEAD].astype(F32), cos, sin).astype(B16) for c in range(0, thin, HEAD)], axis=1)
            qkv_s[own, pl.ds(thin * n, thin)] = t[:BLOCK]
            qkv_s[theirs, pl.ds(thin * n, thin)] = t[BLOCK:]

    keep.wait()
    gx.leave()


def attention(gy, dy_ref, wo_ref, ady_ref, dwo_ref, near_s, far_s, qkv_s, dk_s, dv_s, load_sem, pair_sem, out_sem,
              wo_s, seen_s, do_s, lse_s, top_s, mix_s, pair_s, seent_s, dwo_s, out_s, dq_s):
    load = pltpu.make_async_copy(wo_ref, wo_s, load_sem.at[0])
    load.start()
    rows, wide = qkv_s.shape[0], wo_s.shape[1]
    heads = wo_s.shape[0] // HEAD
    scale = HEAD**-0.5
    bq = SPAN
    ones = jnp.ones((8, bq), B16)

    @pl.loop(0, rows // bq)
    def _(iq):
        mine = part(iq, bq)
        top_s[...] = jnp.full_like(top_s, LOW)
        mix_s[...] = jnp.zeros_like(mix_s)

        def block(j, masked):
            here = part(j, bq)
            scores = [dot(qkv_s[here, head(heads + h)], qkv_s[mine, head(h)], 1, 1) for h in range(heads)]
            if masked:
                seen = lax.broadcasted_iota(jnp.int32, (bq, bq), 1) >= lax.broadcasted_iota(jnp.int32, (bq, bq), 0)
                scores = [jnp.where(seen, s, HIDDEN) for s in scores]
            weights, keeps = [], []
            for h, s in enumerate(scores):
                old = top_s[h : h + 1, :]
                top = jnp.maximum(old, s.max(axis=0, keepdims=True))
                top_s[h : h + 1, :] = top
                weights.append(jnp.exp2((s - top) * E2).astype(B16))
                keeps.append(jnp.exp2((old - top) * E2))
            for h, (p, keep) in enumerate(zip(weights, keeps)):
                values = jnp.concatenate([qkv_s[here, head(2 * heads + h)].T, ones], axis=0)
                mix_s[h] = mix_s[h] * keep + dot(values, p, 1, 0)

        lax.fori_loop(0, iq, lambda j, _: block(j, False), None)
        block(iq, True)
        for h in range(heads):
            total = mix_s[h, HEAD : HEAD + 1, :]
            seen_s[mine, head(h)] = (mix_s[h, :HEAD, :] * (1 / total)).T.astype(B16)
            lse_s[h : h + 1, mine] = top_s[h : h + 1, :] * E2 + jnp.log(total) * LOG2E

    gy.forward(1)
    dwo_s[...] = jnp.zeros_like(dwo_s)
    dk_s[...] = jnp.zeros_like(dk_s)
    dv_s[...] = jnp.zeros_like(dv_s)
    load.wait()

    def back(chip):
        mine = part(chip, UNIT)
        dq_s[...] = jnp.zeros_like(dq_s)
        deltas = [(do_s[mine, head(h)].astype(F32) * seen_s[mine, head(h)].astype(F32)).T.sum(axis=0, keepdims=True) for h in range(heads)]

        def block(j, size, masked):
            here = part(j, size)
            scores = [dot(qkv_s[here, head(heads + h)], qkv_s[mine, head(h)], 1, 1) for h in range(heads)]
            dps = [dot(qkv_s[here, head(2 * heads + h)], do_s[mine, head(h)], 1, 1) for h in range(heads)]
            for h in range(heads):
                p = jnp.exp2(scores[h] * E2 - lse_s[h : h + 1, mine])
                if masked:
                    seen = lax.broadcasted_iota(jnp.int32, (UNIT, UNIT), 1) >= lax.broadcasted_iota(jnp.int32, (UNIT, UNIT), 0)
                    p = jnp.where(seen, p, 0.0)
                ds = (p * (dps[h] - deltas[h])).astype(B16)
                dv_s[here, head(h)] += dot(p.astype(B16), do_s[mine, head(h)], 1, 0)
                dk_s[here, head(h)] += dot(ds, qkv_s[mine, head(h)], 1, 0)
                dq_s[h] += dot(qkv_s[here, head(heads + h)].T, ds, 1, 0)

        lax.fori_loop(0, chip // 2, lambda j, _: block(j, 2 * UNIT, False), None)
        lax.fori_loop(chip // 2 * 2, chip, lambda j, _: block(j, UNIT, False), None)
        block(chip, UNIT, True)
        cos, sin = unit_angles(near_s, far_s, 2 * chip, 2 * chip + 1)
        for h in range(heads):
            dq = (dq_s[h] * scale).T.astype(B16).astype(F32)
            qkv_s[mine, head(h)] = turn(dq, cos, -sin).astype(B16)

    def own_half(m):
        return pltpu.make_async_copy(ady_ref.at[part(gy.blocks(m)[0], BLOCK), :], pair_s.at[pl.ds(0, BLOCK), :], pair_sem.at[0])

    pltpu.make_async_copy(dy_ref, pair_s.at[pl.ds(0, BLOCK), :], pair_sem.at[0]).start()

    def dwo_out(c):
        return pltpu.make_async_copy(out_s.at[lax.rem(c, 2)], dwo_ref.at[:, part(c, SPAN)], out_sem.at[lax.rem(c, 2)])

    @pl.loop(0, STEPS)
    def _(m):
        a, b = gy.blocks(m)
        own, theirs = part(a, BLOCK), part(b, BLOCK)
        their_half = pltpu.make_async_copy(ady_ref.at[theirs, :], pair_s.at[pl.ds(BLOCK, BLOCK), :], pair_sem.at[1])

        @pl.when(m >= 1)
        def _():
            gy.handed(m)

        their_half.start()
        seent_s[...] = jnp.concatenate([seen_s[own, :], seen_s[theirs, :]], axis=0).T
        own_half(m).wait()
        their_half.wait()
        t = dot(pair_s[...], wo_s[...], 1, 1).astype(B16)
        do_s[own, :] = t[:BLOCK]
        do_s[theirs, :] = t[BLOCK:]

        far = (m + 1) // 2

        @pl.loop(0, (1 - lax.rem(m, 2)) * (1 + jnp.minimum(m, 1)) + m // (STEPS - 1))
        def _(side):
            back(gy.chip(far * (2 * side - 1)))

        @pl.when(m < STEPS - 1)
        def _():
            @pl.loop(0, wide // (4 * SPAN))
            def _(c):
                for n in range(4):
                    here = pl.ds(pl.multiple_of(c * 4 * SPAN, 4 * SPAN) + n * SPAN, SPAN)
                    dwo_s[:, here] += dot(seent_s[...], pair_s[:, here], 1, 0)

            @pl.when(m >= 1)
            def _():
                gy.forward(m + 1)

            own_half(m + 1).start()

        @pl.when(m == STEPS - 1)
        def _():
            @pl.loop(0, wide // SPAN)
            def _(c):
                @pl.when(c >= 2)
                def _():
                    dwo_out(c - 2).wait()

                out_s[lax.rem(c, 2)] = (dwo_s[:, part(c, SPAN)] + dot(seent_s[...], pair_s[:, part(c, SPAN)], 1, 0)).astype(B16)
                dwo_out(c).start()

    for c in (wide // SPAN - 2, wide // SPAN - 1):
        dwo_out(c).wait()


def spread(gy, x_ref, dy_ref, gain_s, ws, ax_ref, bx_ref, bg_ref, dws, near_s, far_s, qkv_s, dk_s, dv_s, sib_in, run_in, gall_s,
           load_sem, w_sem, slab_sem, dw_sem, sib_ssem, sib_rsem, run_ssem, run_rsem, g_ssem, g_rsem, sib_free, run_free,
           w_s, slab_s, dw_s, own_s, sib_out, run_out, da_s, x_s, dy_s, gp_s, m_s, scale_s):
    group, me, core, r, way, sib, succ, pred = gy.group, gy.me, gy.core, gy.r, gy.way, gy.sib, gy.succ, gy.pred
    wide, thin = ws[0].shape
    piece = COLS // CHUNKS

    def w_load(n):
        return [pltpu.make_async_copy(w.at[part(n, piece), :], w_s.at[part(n, piece), pl.ds(thin * i, thin)], w_sem.at[i, n])
                for i, w in enumerate(ws)]

    def slab_load(k):
        return pltpu.make_async_copy(ax_ref.at[:, part(k, SLAB)], slab_s.at[lax.rem(k, 2)], slab_sem.at[lax.rem(k, 2)])

    @pl.loop(0, CHUNKS)
    def _(n):
        for c in w_load(n):
            c.start()

    slab_load(0).start()

    @pl.loop(CHUNKS, wide // piece)
    def _(n):
        for c in w_load(n):
            c.start()

    loads = [pltpu.make_async_copy(a, b, load_sem.at[i]) for i, (a, b) in enumerate(((x_ref, x_s), (dy_ref, dy_s)))]
    for c in loads:
        c.start()

    def sib_copy(k):
        a, b = lax.rem(k, 2), lax.rem(k, 4)
        return pltpu.make_async_remote_copy(src_ref=sib_out.at[a], dst_ref=sib_in.at[b], send_sem=sib_ssem.at[a], recv_sem=sib_rsem.at[b],
                                            device_id=sib, device_id_type=MESH)

    def run_copy(k):
        a, b = lax.rem(k, 3), lax.rem(k, 8)
        return pltpu.make_async_remote_copy(src_ref=run_out.at[a], dst_ref=run_in.at[b], send_sem=run_ssem.at[a], recv_sem=run_rsem.at[b],
                                            device_id=succ, device_id_type=MESH)

    def gain_copy(j, n):
        return pltpu.make_async_remote_copy(src_ref=gall_s.at[j, me], dst_ref=gall_s.at[j, me], send_sem=g_ssem.at[j, n], recv_sem=g_rsem.at[j, n],
                                            device_id=(group, lax.rem(me + n, GROUP)), device_id_type=MESH)

    def term(k):
        s, j = k // CHUNKS, lax.rem(k, CHUNKS)
        mine = part(chip_at(lax.rem(r - way * (1 + s) + 16, 8)) * 2 + core, BLOCK)
        theirs = part(chip_at(lax.rem(r + way * (1 + s) + 16, 8)) * 2 + 1 - core, BLOCK)
        lhs = jnp.concatenate([qkv_s[mine, :], qkv_s[theirs, :]], axis=0)

        @pl.when(k >= 2)
        def _():
            sib_copy(k - 2).wait_send()

        @pl.when(k >= 4)
        def _():
            pl.semaphore_wait(sib_free, 1)

        @pl.loop(0, CHUNKS)
        def _(n):
            @pl.when(k < CHUNKS)
            def _():
                for c in w_load(k * CHUNKS + n):
                    c.wait()

            t = dot(lhs, w_s[part(j * CHUNKS + n, piece), :], 1, 1)
            own_s[lax.rem(k, 2), :, part(n, piece)] = t[:BLOCK]
            sib_out[lax.rem(k, 2), :, part(n, piece)] = t[BLOCK:].astype(B16)

        sib_copy(k).start()

    def finish(k):
        sib_copy(k).wait_recv()

        def strips(write, with_run):
            @pl.loop(0, 8)
            def _(i):
                rows = part(i, 16)
                v = own_s[lax.rem(k, 2), rows, :] + sib_in[lax.rem(k, 4), rows, :].astype(F32)
                if with_run:
                    v += run_in[lax.rem(k + 4, 8), rows, :].astype(F32)
                write(rows, v)

        def to_run(rows, v):
            run_out[lax.rem(k, 3), rows, :] = v.astype(B16)

        here = part(lax.rem(k, CHUNKS), COLS)

        def to_da(rows, v):
            da_s[rows, here] = v
            t = v * (x_s[rows, here].astype(F32) * scale_s[rows, :1])
            gp_s[...] += t
            t = t * gain_s[:, here]
            m_s[rows, :] += sum(t[:, c : c + 128] for c in range(0, COLS, 128))

        @pl.when((k >= 3) & (k < SENT))
        def _():
            run_copy(k - 3).wait_send()

        @pl.when(k < 4)
        def _():
            strips(to_run, False)

        @pl.when(k >= 4)
        def _():
            run_copy(k - 4).wait_recv()

            @pl.when(k < SENT)
            def _():
                strips(to_run, True)

            @pl.when(k >= SENT)
            def _():
                gp_s[...] = jnp.zeros_like(gp_s)
                strips(to_da, True)
                j = k - SENT
                share = COLS // 8
                for i in range(8):
                    gall_s[j, me, i : i + 1, :] = jnp.sum(gp_s[:, i * share : (i + 1) * share], axis=0, keepdims=True)
                for n in range(1, GROUP):
                    gain_copy(j, n).start()

            @pl.when(k < SENT - 4)
            def _():
                pl.semaphore_signal(run_free, inc=1, device_id=pred, device_id_type=MESH)

        @pl.when(k < ALL - 4)
        def _():
            pl.semaphore_signal(sib_free, inc=1, device_id=sib, device_id_type=MESH)

        @pl.when(k < SENT)
        def _():
            @pl.when(k >= 8)
            def _():
                pl.semaphore_wait(run_free, 1)

            run_copy(k).start()

    def dw_out(k, i):
        at = lax.rem(k, 2)
        return pltpu.make_async_copy(dw_s.at[at, i], dws[i].at[part(k, SLAB), :], dw_sem.at[at, i])

    def slab(k):
        at = lax.rem(k, 2)
        slab_load(k).wait()

        @pl.when(k + 1 < ALL)
        def _():
            slab_load(k + 1).start()

        @pl.when(k >= 2)
        def _():
            for i in range(3):
                dw_out(k - 2, i).wait()

        t = dot(slab_s[at], qkv_s[...], 0, 0)
        for i in range(3):
            dw_s[at, i] = t[:, thin * i : thin * (i + 1)].astype(B16)
            dw_out(k, i).start()

    def settle(chip):
        here = part(chip, UNIT)
        heads = thin // HEAD
        cos, sin = unit_angles(near_s, far_s, 2 * chip, 2 * chip + 1)
        for h in range(heads):
            dk = (dk_s[here, head(h)] * HEAD**-0.5).astype(B16).astype(F32)
            qkv_s[here, head(heads + h)] = turn(dk, cos, -sin).astype(B16)
            qkv_s[here, head(2 * heads + h)] = dv_s[here, head(h)].astype(B16)

    @pl.loop(0, 2)
    def _(side):
        settle(gy.chip(2 * side - 1))

    term(0)

    @pl.loop(0, ALL)
    def _(k):
        @pl.when(k == 1)
        def _():
            @pl.loop(2, 7)
            def _(far):
                settle(gy.chip(far))

            settle(gy.chip(0))

        @pl.when(k + 1 < ALL)
        def _():
            term(k + 1)

        @pl.loop((ALL * jnp.maximum(k - 2, 0)) // (ALL - 2), (ALL * jnp.maximum(k - 1, 0)) // (ALL - 2))
        def _(n):
            slab(n)

        @pl.when(k == 8)
        def _():
            for c in loads:
                c.wait()
            m_s[...] = jnp.zeros_like(m_s)

            @pl.loop(0, BLOCK // 16)
            def _(i):
                x = x_s[part(i, 16), :].astype(F32)
                scale = lax.rsqrt(jnp.sum(x * x, -1, keepdims=True) * (1 / wide) + 1e-6)
                scale_s[part(i, 16), :] = jnp.broadcast_to(scale, (16, 128))

        finish(k)

    @pl.loop(0, BLOCK // 16)
    def _(i):
        rows = part(i, 16)
        scale = scale_s[rows, :1]
        m = jnp.sum(m_s[rows, :], -1, keepdims=True) * (1 / wide)
        u = da_s[rows, :] * gain_s[...] - x_s[rows, :].astype(F32) * (scale * m)
        x_s[rows, :] = (dy_s[rows, :].astype(F32) + scale * u).astype(B16)
        pltpu.make_async_copy(x_s.at[rows, :], bx_ref.at[rows, :], load_sem.at[i]).start()

    for k in (ALL - 2, ALL - 1):
        for i in range(3):
            dw_out(k, i).wait()
    for k in range(ALL - 2, ALL):
        sib_copy(k).wait_send()
    for k in range(SENT - 3, SENT):
        run_copy(k).wait_send()

    @pl.loop(0, CHUNKS)
    def _(j):
        for n in range(1, GROUP):
            gain_copy(j, n).wait()

    for j in range(CHUNKS):
        v = sum(gall_s[j, n] for n in range(GROUP))
        share = COLS // 8
        for i in range(8):
            bg_ref[:, j * COLS + i * share : j * COLS + (i + 1) * share] = v[i : i + 1, :]
    @pl.loop(0, BLOCK // 16)
    def _(i):
        pltpu.make_async_copy(x_s.at[part(i, 16), :], bx_ref.at[part(i, 16), :], load_sem.at[i]).wait()


def whole_kernel(x_ref, dy_ref, gain_ref, wq_ref, wk_ref, wv_ref, wo_ref, near_ref, far_ref,
                 bx_ref, bg_ref, dwq_ref, dwk_ref, dwv_ref, dwo_ref, ax_ref, ady_ref,
                 gain_raw, gain_s, near_s, far_s, qkv_s, dk_s, dv_s, sib_in, run_in, gall_s, load_sem, w_sem, pair_sem, out_sem, *sems):
    gx_sems, gy_sems, ring_sems = sems[:4], sems[4:8], sems[8:]
    gy = Gather(dy_ref, ady_ref, *gy_sems)
    barrier = pltpu.get_barrier_semaphore()
    for n in range(1, GROUP):
        pl.semaphore_signal(barrier, inc=1, device_id=(gy.group, lax.rem(gy.me + n, GROUP)), device_id_type=MESH)
    small = [pltpu.make_async_copy(a, b, load_sem.at[PIECES + i]) for i, (a, b) in enumerate(((gain_ref, gain_raw), (near_ref, near_s), (far_ref, far_s)))]
    V = pltpu.VMEM
    ws, dws = (wq_ref, wk_ref, wv_ref), (dwq_ref, dwk_ref, dwv_ref)
    wide, thin = wq_ref.shape
    rows = qkv_s.shape[0]
    heads = thin // HEAD
    mine = V((BLOCK, wide), B16)
    pair = V((2, UNIT, wide), B16)
    chunks = lambda n: V((n, BLOCK, COLS), B16)

    def one(x_s, own_s, w_s, pair_s):
        gx = Gather(own_s, ax_ref, *gx_sems)
        project(gx, gy, small, x_ref, gain_raw, gain_s, ws, ax_ref, near_s, far_s, qkv_s, load_sem, w_sem, pair_sem, x_s, own_s, w_s, pair_s)

    pl.run_scoped(one, mine, mine, V((3, wide, thin), B16), pair)

    def two(*refs):
        attention(gy, dy_ref, wo_ref, ady_ref, dwo_ref, near_s, far_s, qkv_s, dk_s, dv_s, load_sem, pair_sem, out_sem, *refs)

    pl.run_scoped(two, V((thin, wide), B16), V((rows, thin), B16), V((rows, thin), B16), V((heads, rows), F32), V((heads, SPAN), F32),
                  V((heads, HEAD + 8, SPAN), F32), V((UNIT, wide), B16), V((thin, UNIT), B16), V((thin, wide), F32), V((2, thin, SPAN), B16),
                  V((heads, HEAD, UNIT), F32))

    def three(*refs):
        spread(gy, x_ref, dy_ref, gain_s, ws, ax_ref, bx_ref, bg_ref, dws, near_s, far_s, qkv_s, dk_s, dv_s, sib_in, run_in, gall_s, load_sem, w_sem, *ring_sems, *refs)

    pl.run_scoped(three, V((wide, 3 * thin), B16), V((2, rows, SLAB), B16), V((2, 3, SLAB, thin), B16), V((2, BLOCK, COLS), F32), chunks(2), chunks(3),
                  V((BLOCK, wide), F32), mine, mine, V((16, COLS), F32), V((BLOCK, 128), F32), V((BLOCK, 128), F32))
    gy.leave()


def whole(x, dy, gain, wq, wk, wv, wo):
    block, wide = x.shape
    rows, thin = GROUP * block, wq.shape[1]
    V, D = pltpu.VMEM, lambda *shape: pltpu.SemaphoreType.DMA(shape)
    S = jax.ShapeDtypeStruct
    near, far = tables()
    sem = pltpu.SemaphoreType.REGULAR
    bx, bg, *dw, _, _ = pl.pallas_call(
        whole_kernel,
        out_shape=[S(x.shape, B16), S((1, wide), F32)] + [S(wq.shape, B16)] * 3 + [S(wo.shape, B16)] + [S((rows, wide), B16)] * 2,
        in_specs=[ANY] * 9,
        out_specs=[ANY, VM] + [ANY] * 6,
        scratch_shapes=[V(gain.shape, B16), V((1, wide), F32), V(near.shape, F32), V(far.shape, F32), V((rows, 3 * thin), B16), V((rows, thin), F32), V((rows, thin), F32),
                        V((4, block, COLS), B16),                        V((8, block, COLS), B16), V((CHUNKS, GROUP, 8, COLS // 8), F32), D(8), D(3, 16), D(2), D(2)]
                       + [D(STEPS, PIECES)] * 8
                       + [D(2), D(2, 3), D(4), D(4), D(4), D(8), D(CHUNKS, GROUP), D(CHUNKS, GROUP), sem, sem],
        compiler_params=pltpu.CompilerParams(collective_id=0, has_side_effects=True, vmem_limit_bytes=LIMIT),
        cost_estimate=pl.CostEstimate(flops=22 * rows * thin * wide, bytes_accessed=8 * rows * wide, transcendentals=0),
        name="whole",
    )(x, dy, gain, wq, wk, wv, wo, near, far)
    steps = 8
    given = [bx, *dw]
    specs = [pl.BlockSpec((g.shape[0] // steps, g.shape[1]), lambda i: (i, 0)) for g in given] + [pl.BlockSpec(bg.shape, lambda i: (0, 0))]
    bx, *dw, bg = pl.pallas_call(copy_kernel, grid=(steps,), in_specs=specs, out_specs=specs, out_shape=[S(g.shape, g.dtype) for g in (*given, bg)],
                                 compiler_params=pltpu.CompilerParams(vmem_limit_bytes=LIMIT), name="results")(*given, bg)
    return bx, bg, *dw


def solution(mesh):
    def step(x, dy, gain, wq, wk, wv, wo):
        gain = gain.reshape(-1, HEAD)
        return whole(x, dy, gain, wq, wk, wv, wo)

    tokens, columns = P(("dp", "tp"), None), P(None, "tp")
    return jax.shard_map(
        step,
        mesh=mesh,
        in_specs=(tokens, tokens, P(None), columns, columns, columns, P("tp", None)),
        out_specs=(tokens, P("dp", None), P("dp", "tp"), P("dp", "tp"), P("dp", "tp"), P(("dp", "tp"), None)),
        check_vma=False,
    )
```

```python
import jax
import jax.numpy as jnp
import numpy as np
from jax import lax
from jax.experimental import pallas as pl
from jax.experimental.pallas import tpu as pltpu
from jax.sharding import PartitionSpec as P

HEAD = 128
LOW = -1e30
HIDDEN = 2 * LOW
LOG2E = 1.4426950408889634
E2 = HEAD**-0.5 * LOG2E


def dot(a, b, ca, cb):
    return lax.dot_general(a, b, (((ca,), (cb,)), ((), ())), preferred_element_type=jnp.float32)


def head(h):
    return pl.ds(HEAD * h, HEAD)


def turn(t, cos, sin):
    half = HEAD // 2
    return t * cos + jnp.concatenate([t[:, half:], t[:, :half]], axis=1) * sin


def tables():
    rate = 10000.0 ** -(np.arange(HEAD) % (HEAD // 2) / (HEAD // 2))
    sign = np.where(np.arange(HEAD) < HEAD // 2, -1.0, 1.0)
    near, far = np.arange(128)[:, None] * rate, 128 * np.arange(16)[:, None] * rate
    return tuple(jnp.asarray(np.stack([np.cos(t), np.sin(t) * sign]), jnp.float32) for t in (near, far))


def angles(near_ref, far_ref, block):
    c, s = far_ref[0, pl.ds(block, 1), :], far_ref[1, pl.ds(block, 1), :]
    return near_ref[0] * c - near_ref[1] * s, near_ref[1] * c + near_ref[0] * s


def unit_angles(near_ref, far_ref, a, b):
    return tuple(jnp.concatenate(t, axis=0) for t in zip(angles(near_ref, far_ref, a), angles(near_ref, far_ref, b)))


MESH = pl.DeviceIdType.MESH
ANY = pl.BlockSpec(memory_space=pl.ANY)
VM = pl.BlockSpec(memory_space=pltpu.VMEM)
B16, F32 = jnp.bfloat16, jnp.float32
LIMIT = 67043328
GROUP = 16
BLOCK = 128


def dot(a, b, ca, cb):
    return lax.dot_general(a, b, (((ca,), (cb,)), ((), ())), preferred_element_type=jnp.float32)


def chip_at(r):
    far = r // 4
    return r * (1 - far) + (11 - r) * far


def part(i, size):
    return pl.ds(pl.multiple_of(i * size, size), size)


COLS = 2048
SLAB = 256
CHUNKS = 4
SENT = 7 * CHUNKS
ALL = 8 * CHUNKS


def copy_kernel(*refs):
    half = len(refs) // 2
    for a, b in zip(refs[:half], refs[half:]):
        b[...] = a[...]


UNIT = 2 * BLOCK
STEPS = 8
PIECES = 4
SPAN = 512


class Gather:
    def __init__(self, own_ref, out_ref, send_sem, recv_sem, sib_ssem, sib_rsem):
        self.own_ref, self.out_ref = own_ref, out_ref
        self.sems = send_sem, recv_sem, sib_ssem, sib_rsem
        group, me = lax.axis_index("dp"), lax.axis_index("tp")
        self.group, self.me = group, me
        self.core, self.r = lax.rem(me, 2), chip_at(me // 2)
        self.way = 1 - 2 * self.core
        self.sib = (group, me + self.way)
        self.succ, self.pred = ((group, chip_at(lax.rem(self.r + to + 8, 8)) * 2 + self.core) for to in (self.way, -self.way))

    def chip(self, far):
        return chip_at(lax.rem(self.r + far * self.way + 16, 8))

    def blocks(self, m):
        far, odd = (m + 1) // 2, lax.rem(m + 1, 2) * jnp.minimum(m, 1)
        return self.chip(-far) * 2 + self.core + odd * self.way, self.chip(far) * 2 + 1 - self.core - odd * self.way

    def copy(self, place, p, own, sems, m, to):
        there = self.out_ref.at[part(place * PIECES + p, BLOCK // PIECES), :]
        src = self.own_ref.at[part(p, BLOCK // PIECES), :] if own else there
        return pltpu.make_async_remote_copy(src_ref=src, dst_ref=there, send_sem=self.sems[sems].at[m, p], recv_sem=self.sems[sems + 1].at[m, p],
                                            device_id=to, device_id_type=MESH)

    def ring(self, m, p, own=False):
        far, odd = (m - 1) // 2, lax.rem(m - 1, 2)
        return self.copy(self.chip(-far) * 2 + self.core + odd * self.way, p, own, 0, m, self.succ)

    def hand(self, m, p, own=False):
        return self.copy(self.blocks(m)[0], p, own, 2, m, self.sib)

    def start(self, p):
        self.ring(1, p, True).start()
        self.hand(0, p, True).start()

    def forward(self, m):
        @pl.loop(0, PIECES)
        def _(p):
            self.ring(m, p).wait_recv()
            self.hand(m, p).start()

            @pl.when(m + 2 < STEPS)
            def _():
                self.ring(m + 2, p).start()

    def first(self):
        @pl.loop(0, PIECES)
        def _(p):
            self.hand(0, p, True).wait_recv()
            self.ring(2, p).start()

    def handed(self, m):
        @pl.loop(0, PIECES)
        def _(p):
            self.hand(m, p).wait_recv()

    def leave(self):
        @pl.loop(0, PIECES)
        def _(p):
            self.ring(1, p, True).wait_send()
            self.hand(0, p, True).wait_send()

            @pl.loop(1, STEPS)
            def _(m):
                self.hand(m, p).wait_send()

                @pl.when(m >= 2)
                def _():
                    self.ring(m, p).wait_send()


def project(gx, gy, small, x_ref, gain_raw, gain_s, ws, ax_ref, near_s, far_s, qkv_s, load_sem, w_sem, pair_sem, x_s, own_s, w_s, pair_s):
    wide, thin = ws[0].shape
    rows = BLOCK // PIECES
    load = [pltpu.make_async_copy(x_ref.at[part(p, rows), :], x_s.at[part(p, rows), :], load_sem.at[p]) for p in range(PIECES)]
    for c in load:
        c.start()
    for c in small:
        c.start()
    w_load = [pltpu.make_async_copy(w, w_s.at[n], w_sem.at[n, 0]) for n, w in enumerate(ws)]
    for c in w_load:
        c.start()
    for c in small:
        c.wait()
    gain = gain_raw[...].astype(F32)
    for n in range(wide // HEAD):
        gain_s[:, HEAD * n : HEAD * (n + 1)] = gain[n : n + 1, :]
    for p in range(PIECES):
        load[p].wait()

        @pl.loop(p * rows // 16, (p + 1) * rows // 16)
        def _(i):
            x = x_s[part(i, 16), :].astype(F32)
            scale = lax.rsqrt(jnp.sum(x * x, -1, keepdims=True) * (1 / wide) + 1e-6)
            a = (x * scale * gain_s[...]).astype(B16)
            own_s[part(i, 16), :] = a
            pair_s[0, part(i, 16), :] = a

        if p == 0:
            pl.semaphore_wait(pltpu.get_barrier_semaphore(), GROUP - 1)
        gx.start(p)
    keep = pltpu.make_async_copy(own_s, ax_ref.at[part(gx.me, BLOCK), :], load_sem.at[0])
    keep.start()
    gx.first()

    @pl.loop(0, STEPS)
    def _(m):
        at = lax.rem(m, 2)
        a, b = gx.blocks(m)
        own, theirs = part(a, BLOCK), part(b, BLOCK)
        halves = [pltpu.make_async_copy(ax_ref.at[there, :], pair_s.at[at, pl.ds(n * BLOCK, BLOCK), :], pair_sem.at[n])
                  for n, there in enumerate((own, theirs))]

        @pl.when(m >= 1)
        def _():
            gx.forward(m)
            halves[0].start()

        @pl.when(m == STEPS - 3)
        def _():
            for p in range(PIECES):
                gy.start(p)

        @pl.when(m == STEPS - 2)
        def _():
            gy.first()

        @pl.when(m >= 1)
        def _():
            gx.handed(m)

        halves[1].start()

        @pl.when(m == 0)
        def _():
            for c in w_load:
                c.wait()

        @pl.when(m >= 1)
        def _():
            halves[0].wait()

        halves[1].wait()
        cos, sin = unit_angles(near_s, far_s, a, b)
        for n in range(3):
            t = dot(pair_s[at], w_s[n], 1, 0).astype(B16)
            if n < 2:
                t = jnp.concatenate([turn(t[:, c : c + HEAD].astype(F32), cos, sin).astype(B16) for c in range(0, thin, HEAD)], axis=1)
            qkv_s[own, pl.ds(thin * n, thin)] = t[:BLOCK]
            qkv_s[theirs, pl.ds(thin * n, thin)] = t[BLOCK:]

    keep.wait()
    gx.leave()


def attention(gy, dy_ref, wo_ref, ady_ref, dwo_ref, near_s, far_s, qkv_s, dk_s, dv_s, load_sem, pair_sem, out_sem,
              wo_s, seen_s, do_s, lse_s, top_s, mix_s, pair_s, seent_s, dwo_s, out_s, dq_s):
    load = pltpu.make_async_copy(wo_ref, wo_s, load_sem.at[0])
    load.start()
    rows, wide = qkv_s.shape[0], wo_s.shape[1]
    heads = wo_s.shape[0] // HEAD
    scale = HEAD**-0.5
    bq = SPAN
    ones = jnp.ones((8, bq), B16)

    @pl.loop(0, rows // bq)
    def _(iq):
        mine = part(iq, bq)
        top_s[...] = jnp.full_like(top_s, LOW)
        mix_s[...] = jnp.zeros_like(mix_s)

        def block(j, masked):
            here = part(j, bq)
            scores = [dot(qkv_s[here, head(heads + h)], qkv_s[mine, head(h)], 1, 1) for h in range(heads)]
            if masked:
                seen = lax.broadcasted_iota(jnp.int32, (bq, bq), 1) >= lax.broadcasted_iota(jnp.int32, (bq, bq), 0)
                scores = [jnp.where(seen, s, HIDDEN) for s in scores]
            weights, keeps = [], []
            for h, s in enumerate(scores):
                old = top_s[h : h + 1, :]
                top = jnp.maximum(old, s.max(axis=0, keepdims=True))
                top_s[h : h + 1, :] = top
                weights.append(jnp.exp2((s - top) * E2).astype(B16))
                keeps.append(jnp.exp2((old - top) * E2))
            for h, (p, keep) in enumerate(zip(weights, keeps)):
                values = jnp.concatenate([qkv_s[here, head(2 * heads + h)].T, ones], axis=0)
                mix_s[h] = mix_s[h] * keep + dot(values, p, 1, 0)

        lax.fori_loop(0, iq, lambda j, _: block(j, False), None)
        block(iq, True)
        for h in range(heads):
            total = mix_s[h, HEAD : HEAD + 1, :]
            seen_s[mine, head(h)] = (mix_s[h, :HEAD, :] * (1 / total)).T.astype(B16)
            lse_s[h : h + 1, mine] = top_s[h : h + 1, :] * E2 + jnp.log(total) * LOG2E

    gy.forward(1)
    dwo_s[...] = jnp.zeros_like(dwo_s)
    dk_s[...] = jnp.zeros_like(dk_s)
    dv_s[...] = jnp.zeros_like(dv_s)
    load.wait()

    def back(chip):
        mine = part(chip, UNIT)
        dq_s[...] = jnp.zeros_like(dq_s)
        deltas = [(do_s[mine, head(h)].astype(F32) * seen_s[mine, head(h)].astype(F32)).T.sum(axis=0, keepdims=True) for h in range(heads)]

        def block(j, size, masked):
            here = part(j, size)
            scores = [dot(qkv_s[here, head(heads + h)], qkv_s[mine, head(h)], 1, 1) for h in range(heads)]
            dps = [dot(qkv_s[here, head(2 * heads + h)], do_s[mine, head(h)], 1, 1) for h in range(heads)]
            for h in range(heads):
                p = jnp.exp2(scores[h] * E2 - lse_s[h : h + 1, mine])
                if masked:
                    seen = lax.broadcasted_iota(jnp.int32, (UNIT, UNIT), 1) >= lax.broadcasted_iota(jnp.int32, (UNIT, UNIT), 0)
                    p = jnp.where(seen, p, 0.0)
                ds = (p * (dps[h] - deltas[h])).astype(B16)
                dv_s[here, head(h)] += dot(p.astype(B16), do_s[mine, head(h)], 1, 0)
                dk_s[here, head(h)] += dot(ds, qkv_s[mine, head(h)], 1, 0)
                dq_s[h] += dot(qkv_s[here, head(heads + h)].T, ds, 1, 0)

        lax.fori_loop(0, chip // 2, lambda j, _: block(j, 2 * UNIT, False), None)
        lax.fori_loop(chip // 2 * 2, chip, lambda j, _: block(j, UNIT, False), None)
        block(chip, UNIT, True)
        cos, sin = unit_angles(near_s, far_s, 2 * chip, 2 * chip + 1)
        for h in range(heads):
            dq = (dq_s[h] * scale).T.astype(B16).astype(F32)
            qkv_s[mine, head(h)] = turn(dq, cos, -sin).astype(B16)

    def own_half(m):
        return pltpu.make_async_copy(ady_ref.at[part(gy.blocks(m)[0], BLOCK), :], pair_s.at[pl.ds(0, BLOCK), :], pair_sem.at[0])

    pltpu.make_async_copy(dy_ref, pair_s.at[pl.ds(0, BLOCK), :], pair_sem.at[0]).start()

    def dwo_out(c):
        return pltpu.make_async_copy(out_s.at[lax.rem(c, 2)], dwo_ref.at[:, part(c, SPAN)], out_sem.at[lax.rem(c, 2)])

    @pl.loop(0, STEPS)
    def _(m):
        a, b = gy.blocks(m)
        own, theirs = part(a, BLOCK), part(b, BLOCK)
        their_half = pltpu.make_async_copy(ady_ref.at[theirs, :], pair_s.at[pl.ds(BLOCK, BLOCK), :], pair_sem.at[1])

        @pl.when(m >= 1)
        def _():
            gy.handed(m)

        their_half.start()
        seent_s[...] = jnp.concatenate([seen_s[own, :], seen_s[theirs, :]], axis=0).T
        own_half(m).wait()
        their_half.wait()
        t = dot(pair_s[...], wo_s[...], 1, 1).astype(B16)
        do_s[own, :] = t[:BLOCK]
        do_s[theirs, :] = t[BLOCK:]

        far = (m + 1) // 2

        @pl.loop(0, (1 - lax.rem(m, 2)) * (1 + jnp.minimum(m, 1)) + m // (STEPS - 1))
        def _(side):
            back(gy.chip(far * (2 * side - 1)))

        @pl.when(m < STEPS - 1)
        def _():
            @pl.loop(0, wide // (4 * SPAN))
            def _(c):
                for n in range(4):
                    here = pl.ds(pl.multiple_of(c * 4 * SPAN, 4 * SPAN) + n * SPAN, SPAN)
                    dwo_s[:, here] += dot(seent_s[...], pair_s[:, here], 1, 0)

            @pl.when(m >= 1)
            def _():
                gy.forward(m + 1)

            own_half(m + 1).start()

        @pl.when(m == STEPS - 1)
        def _():
            @pl.loop(0, wide // SPAN)
            def _(c):
                @pl.when(c >= 2)
                def _():
                    dwo_out(c - 2).wait()

                out_s[lax.rem(c, 2)] = (dwo_s[:, part(c, SPAN)] + dot(seent_s[...], pair_s[:, part(c, SPAN)], 1, 0)).astype(B16)
                dwo_out(c).start()

    for c in (wide // SPAN - 2, wide // SPAN - 1):
        dwo_out(c).wait()


def spread(gy, x_ref, dy_ref, gain_s, ws, ax_ref, bx_ref, bg_ref, dws, near_s, far_s, qkv_s, dk_s, dv_s, sib_in, run_in, gall_s,
           load_sem, w_sem, slab_sem, dw_sem, sib_ssem, sib_rsem, run_ssem, run_rsem, g_ssem, g_rsem, sib_free, run_free,
           w_s, slab_s, dw_s, own_s, sib_out, run_out, da_s, x_s, dy_s, gp_s, m_s, scale_s):
    group, me, core, r, way, sib, succ, pred = gy.group, gy.me, gy.core, gy.r, gy.way, gy.sib, gy.succ, gy.pred
    wide, thin = ws[0].shape
    piece = COLS // CHUNKS

    def w_load(n):
        return [pltpu.make_async_copy(w.at[part(n, piece), :], w_s.at[part(n, piece), pl.ds(thin * i, thin)], w_sem.at[i, n])
                for i, w in enumerate(ws)]

    def slab_load(k):
        return pltpu.make_async_copy(ax_ref.at[:, part(k, SLAB)], slab_s.at[lax.rem(k, 2)], slab_sem.at[lax.rem(k, 2)])

    @pl.loop(0, CHUNKS)
    def _(n):
        for c in w_load(n):
            c.start()

    slab_load(0).start()

    @pl.loop(CHUNKS, wide // piece)
    def _(n):
        for c in w_load(n):
            c.start()

    loads = [pltpu.make_async_copy(a, b, load_sem.at[i]) for i, (a, b) in enumerate(((x_ref, x_s), (dy_ref, dy_s)))]
    for c in loads:
        c.start()

    def sib_copy(k):
        a, b = lax.rem(k, 2), lax.rem(k, 4)
        return pltpu.make_async_remote_copy(src_ref=sib_out.at[a], dst_ref=sib_in.at[b], send_sem=sib_ssem.at[a], recv_sem=sib_rsem.at[b],
                                            device_id=sib, device_id_type=MESH)

    def run_copy(k):
        a, b = lax.rem(k, 3), lax.rem(k, 8)
        return pltpu.make_async_remote_copy(src_ref=run_out.at[a], dst_ref=run_in.at[b], send_sem=run_ssem.at[a], recv_sem=run_rsem.at[b],
                                            device_id=succ, device_id_type=MESH)

    def gain_copy(j, n):
        return pltpu.make_async_remote_copy(src_ref=gall_s.at[j, me], dst_ref=gall_s.at[j, me], send_sem=g_ssem.at[j, n], recv_sem=g_rsem.at[j, n],
                                            device_id=(group, lax.rem(me + n, GROUP)), device_id_type=MESH)

    def term(k):
        s, j = k // CHUNKS, lax.rem(k, CHUNKS)
        mine = part(chip_at(lax.rem(r - way * (1 + s) + 16, 8)) * 2 + core, BLOCK)
        theirs = part(chip_at(lax.rem(r + way * (1 + s) + 16, 8)) * 2 + 1 - core, BLOCK)
        lhs = jnp.concatenate([qkv_s[mine, :], qkv_s[theirs, :]], axis=0)

        @pl.when(k >= 2)
        def _():
            sib_copy(k - 2).wait_send()

        @pl.when(k >= 4)
        def _():
            pl.semaphore_wait(sib_free, 1)

        @pl.loop(0, CHUNKS)
        def _(n):
            @pl.when(k < CHUNKS)
            def _():
                for c in w_load(k * CHUNKS + n):
                    c.wait()

            t = dot(lhs, w_s[part(j * CHUNKS + n, piece), :], 1, 1)
            own_s[lax.rem(k, 2), :, part(n, piece)] = t[:BLOCK]
            sib_out[lax.rem(k, 2), :, part(n, piece)] = t[BLOCK:].astype(B16)

        sib_copy(k).start()

    def finish(k):
        sib_copy(k).wait_recv()

        def strips(write, with_run):
            @pl.loop(0, 8)
            def _(i):
                rows = part(i, 16)
                v = own_s[lax.rem(k, 2), rows, :] + sib_in[lax.rem(k, 4), rows, :].astype(F32)
                if with_run:
                    v += run_in[lax.rem(k + 4, 8), rows, :].astype(F32)
                write(rows, v)

        def to_run(rows, v):
            run_out[lax.rem(k, 3), rows, :] = v.astype(B16)

        here = part(lax.rem(k, CHUNKS), COLS)

        def to_da(rows, v):
            da_s[rows, here] = v
            t = v * (x_s[rows, here].astype(F32) * scale_s[rows, :1])
            gp_s[...] += t
            t = t * gain_s[:, here]
            m_s[rows, :] += sum(t[:, c : c + 128] for c in range(0, COLS, 128))

        @pl.when((k >= 3) & (k < SENT))
        def _():
            run_copy(k - 3).wait_send()

        @pl.when(k < 4)
        def _():
            strips(to_run, False)

        @pl.when(k >= 4)
        def _():
            run_copy(k - 4).wait_recv()

            @pl.when(k < SENT)
            def _():
                strips(to_run, True)

            @pl.when(k >= SENT)
            def _():
                gp_s[...] = jnp.zeros_like(gp_s)
                strips(to_da, True)
                j = k - SENT
                v = jnp.sum(gp_s[...], axis=0, keepdims=True)
                gall_s[j, me] = jnp.concatenate([v[:, i : i + 128] for i in range(0, COLS, 128)], axis=0).astype(B16)
                for n in range(1, GROUP):
                    gain_copy(j, n).start()

            @pl.when(k < SENT - 4)
            def _():
                pl.semaphore_signal(run_free, inc=1, device_id=pred, device_id_type=MESH)

        @pl.when(k < ALL - 4)
        def _():
            pl.semaphore_signal(sib_free, inc=1, device_id=sib, device_id_type=MESH)

        @pl.when(k < SENT)
        def _():
            @pl.when(k >= 8)
            def _():
                pl.semaphore_wait(run_free, 1)

            run_copy(k).start()

    def dw_out(k, i):
        at = lax.rem(k, 2)
        return pltpu.make_async_copy(dw_s.at[at, i], dws[i].at[part(k, SLAB), :], dw_sem.at[at, i])

    def slab(k):
        at = lax.rem(k, 2)
        slab_load(k).wait()

        @pl.when(k + 1 < ALL)
        def _():
            slab_load(k + 1).start()

        @pl.when(k >= 2)
        def _():
            for i in range(3):
                dw_out(k - 2, i).wait()

        t = dot(slab_s[at], qkv_s[...], 0, 0)
        for i in range(3):
            dw_s[at, i] = t[:, thin * i : thin * (i + 1)].astype(B16)
            dw_out(k, i).start()

    def settle(chip):
        here = part(chip, UNIT)
        heads = thin // HEAD
        cos, sin = unit_angles(near_s, far_s, 2 * chip, 2 * chip + 1)
        for h in range(heads):
            dk = (dk_s[here, head(h)] * HEAD**-0.5).astype(B16).astype(F32)
            qkv_s[here, head(heads + h)] = turn(dk, cos, -sin).astype(B16)
            qkv_s[here, head(2 * heads + h)] = dv_s[here, head(h)].astype(B16)

    @pl.loop(0, 2)
    def _(side):
        settle(gy.chip(2 * side - 1))

    term(0)

    @pl.loop(0, ALL)
    def _(k):
        @pl.when(k == 1)
        def _():
            @pl.loop(2, 7)
            def _(far):
                settle(gy.chip(far))

            settle(gy.chip(0))

        @pl.when(k + 1 < ALL)
        def _():
            term(k + 1)

        @pl.loop((ALL * jnp.maximum(k - 2, 0)) // (ALL - 2), (ALL * jnp.maximum(k - 1, 0)) // (ALL - 2))
        def _(n):
            slab(n)

        @pl.when(k == 8)
        def _():
            for c in loads:
                c.wait()
            m_s[...] = jnp.zeros_like(m_s)

            @pl.loop(0, BLOCK // 16)
            def _(i):
                x = x_s[part(i, 16), :].astype(F32)
                scale = lax.rsqrt(jnp.sum(x * x, -1, keepdims=True) * (1 / wide) + 1e-6)
                scale_s[part(i, 16), :] = jnp.broadcast_to(scale, (16, 128))

        finish(k)

    @pl.loop(0, BLOCK // 16)
    def _(i):
        rows = part(i, 16)
        scale = scale_s[rows, :1]
        m = jnp.sum(m_s[rows, :], -1, keepdims=True) * (1 / wide)
        u = da_s[rows, :] * gain_s[...] - x_s[rows, :].astype(F32) * (scale * m)
        x_s[rows, :] = (dy_s[rows, :].astype(F32) + scale * u).astype(B16)
        pltpu.make_async_copy(x_s.at[rows, :], bx_ref.at[rows, :], load_sem.at[i]).start()

    for k in (ALL - 2, ALL - 1):
        for i in range(3):
            dw_out(k, i).wait()
    for k in range(ALL - 2, ALL):
        sib_copy(k).wait_send()
    for k in range(SENT - 3, SENT):
        run_copy(k).wait_send()

    @pl.loop(0, CHUNKS)
    def _(j):
        for n in range(1, GROUP):
            gain_copy(j, n).wait()

    for j in range(CHUNKS):
        v = sum(gall_s[j, n].astype(F32) for n in range(GROUP))
        for i in range(COLS // 128):
            bg_ref[:, j * COLS + i * 128 : j * COLS + (i + 1) * 128] = v[i : i + 1, :]
    @pl.loop(0, BLOCK // 16)
    def _(i):
        pltpu.make_async_copy(x_s.at[part(i, 16), :], bx_ref.at[part(i, 16), :], load_sem.at[i]).wait()


def whole_kernel(x_ref, dy_ref, gain_ref, wq_ref, wk_ref, wv_ref, wo_ref, near_ref, far_ref,
                 bx_ref, bg_ref, dwq_ref, dwk_ref, dwv_ref, dwo_ref, ax_ref, ady_ref,
                 gain_raw, gain_s, near_s, far_s, qkv_s, dk_s, dv_s, sib_in, run_in, gall_s, load_sem, w_sem, pair_sem, out_sem, *sems):
    gx_sems, gy_sems, ring_sems = sems[:4], sems[4:8], sems[8:]
    gy = Gather(dy_ref, ady_ref, *gy_sems)
    barrier = pltpu.get_barrier_semaphore()
    for n in range(1, GROUP):
        pl.semaphore_signal(barrier, inc=1, device_id=(gy.group, lax.rem(gy.me + n, GROUP)), device_id_type=MESH)
    small = [pltpu.make_async_copy(a, b, load_sem.at[PIECES + i]) for i, (a, b) in enumerate(((gain_ref, gain_raw), (near_ref, near_s), (far_ref, far_s)))]
    V = pltpu.VMEM
    ws, dws = (wq_ref, wk_ref, wv_ref), (dwq_ref, dwk_ref, dwv_ref)
    wide, thin = wq_ref.shape
    rows = qkv_s.shape[0]
    heads = thin // HEAD
    mine = V((BLOCK, wide), B16)
    pair = V((2, UNIT, wide), B16)
    chunks = lambda n: V((n, BLOCK, COLS), B16)

    def one(x_s, own_s, w_s, pair_s):
        gx = Gather(own_s, ax_ref, *gx_sems)
        project(gx, gy, small, x_ref, gain_raw, gain_s, ws, ax_ref, near_s, far_s, qkv_s, load_sem, w_sem, pair_sem, x_s, own_s, w_s, pair_s)

    pl.run_scoped(one, mine, mine, V((3, wide, thin), B16), pair)

    def two(*refs):
        attention(gy, dy_ref, wo_ref, ady_ref, dwo_ref, near_s, far_s, qkv_s, dk_s, dv_s, load_sem, pair_sem, out_sem, *refs)

    pl.run_scoped(two, V((thin, wide), B16), V((rows, thin), B16), V((rows, thin), B16), V((heads, rows), F32), V((heads, SPAN), F32),
                  V((heads, HEAD + 8, SPAN), F32), V((UNIT, wide), B16), V((thin, UNIT), B16), V((thin, wide), F32), V((2, thin, SPAN), B16),
                  V((heads, HEAD, UNIT), F32))

    def three(*refs):
        spread(gy, x_ref, dy_ref, gain_s, ws, ax_ref, bx_ref, bg_ref, dws, near_s, far_s, qkv_s, dk_s, dv_s, sib_in, run_in, gall_s, load_sem, w_sem, *ring_sems, *refs)

    pl.run_scoped(three, V((wide, 3 * thin), B16), V((2, rows, SLAB), B16), V((2, 3, SLAB, thin), B16), V((2, BLOCK, COLS), F32), chunks(2), chunks(3),
                  V((BLOCK, wide), F32), mine, mine, V((16, COLS), F32), V((BLOCK, 128), F32), V((BLOCK, 128), F32))
    gy.leave()


def whole(x, dy, gain, wq, wk, wv, wo):
    block, wide = x.shape
    rows, thin = GROUP * block, wq.shape[1]
    V, D = pltpu.VMEM, lambda *shape: pltpu.SemaphoreType.DMA(shape)
    S = jax.ShapeDtypeStruct
    near, far = tables()
    sem = pltpu.SemaphoreType.REGULAR
    bx, bg, *dw, _, _ = pl.pallas_call(
        whole_kernel,
        out_shape=[S(x.shape, B16), S((1, wide), F32)] + [S(wq.shape, B16)] * 3 + [S(wo.shape, B16)] + [S((rows, wide), B16)] * 2,
        in_specs=[ANY] * 9,
        out_specs=[ANY, VM] + [ANY] * 6,
        scratch_shapes=[V(gain.shape, B16), V((1, wide), F32), V(near.shape, F32), V(far.shape, F32), V((rows, 3 * thin), B16), V((rows, thin), F32), V((rows, thin), F32),
                        V((4, block, COLS), B16),                        V((8, block, COLS), B16), V((CHUNKS, GROUP, COLS // 128, 128), B16), D(8), D(3, 16), D(2), D(2)]
                       + [D(STEPS, PIECES)] * 8
                       + [D(2), D(2, 3), D(4), D(4), D(4), D(8), D(CHUNKS, GROUP), D(CHUNKS, GROUP), sem, sem],
        compiler_params=pltpu.CompilerParams(collective_id=0, has_side_effects=True, vmem_limit_bytes=LIMIT),
        cost_estimate=pl.CostEstimate(flops=22 * rows * thin * wide, bytes_accessed=8 * rows * wide, transcendentals=0),
        name="whole",
    )(x, dy, gain, wq, wk, wv, wo, near, far)
    steps = 8
    given = [bx, *dw]
    specs = [pl.BlockSpec((g.shape[0] // steps, g.shape[1]), lambda i: (i, 0)) for g in given] + [pl.BlockSpec(bg.shape, lambda i: (0, 0))]
    bx, *dw, bg = pl.pallas_call(copy_kernel, grid=(steps,), in_specs=specs, out_specs=specs, out_shape=[S(g.shape, g.dtype) for g in (*given, bg)],
                                 compiler_params=pltpu.CompilerParams(vmem_limit_bytes=LIMIT), name="results")(*given, bg)
    return bx, bg, *dw


def solution(mesh):
    def step(x, dy, gain, wq, wk, wv, wo):
        gain = gain.reshape(-1, HEAD)
        return whole(x, dy, gain, wq, wk, wv, wo)

    tokens, columns = P(("dp", "tp"), None), P(None, "tp")
    return jax.shard_map(
        step,
        mesh=mesh,
        in_specs=(tokens, tokens, P(None), columns, columns, columns, P("tp", None)),
        out_specs=(tokens, P("dp", None), P("dp", "tp"), P("dp", "tp"), P("dp", "tp"), P(("dp", "tp"), None)),
        check_vma=False,
    )
```
